512 devices in a mesh: groups: 2 (over y), seq: 16 (over z), tensor: 8 (over x), sub: 2 (over core).
Axes of the slice: x: 8, y: 2, z: 16, core: 2. Of those that a mesh axis runs over, the one named last changes fastest.
The devices are a block of a 8x8x16 slice.
Arguments:
- image_tokens: bfloat16 [8192, 3072], P(('groups', 'seq')), parts along dimension 0, may hold values from -6 to 6
- text_tokens: bfloat16 [1024, 3072], P(('groups', 'seq')), parts along dimension 0, may hold values from -6 to 6
- timestep: int32 [2], P('groups'), parts along dimension 0, may hold values from 0 to 49
- text_length: int32 [2], P('groups'), parts along dimension 0, may hold values from 128 to 512
- time_table: bfloat16 [50, 3072], replicated, may hold values from -6 to 6
- mod_weight: bfloat16 [3072, 18432], P('seq', ('tensor', 'sub')), may hold values from -0.109375 to 0.109375
- qkv_image: bfloat16 [3072, 6144], P('seq', ('tensor', 'sub')), as said below
- qkv_text: bfloat16 [3072, 6144], P('seq', ('tensor', 'sub')), as said below
- norm_gain: float32 [2, 2, 16, 128], P(None, None, ('tensor', 'sub')), may hold values from 1 to 6
- proj_image: bfloat16 [2048, 3072], P(('tensor', 'sub'), 'seq'), may hold values from -0.125 to 0.125
- proj_text: bfloat16 [2048, 3072], P(('tensor', 'sub'), 'seq'), may hold values from -0.125 to 0.125
Outputs:
- image_out: bfloat16 [8192, 3072], P(('groups', 'seq'), ('tensor', 'sub')), parts along dimension 0
- text_out: bfloat16 [1024, 3072], P(('groups', 'seq'), ('tensor', 'sub')), parts along dimension 0
The draws below stay inside these ranges and needn't reach their ends.
There are 2 independent parts, one for each index of `groups`. The reference program is written for one: setup_inputs(seed, part) draws one part's arguments, and reference() takes and returns one part's arrays. A program takes and returns all parts, laid end to end along the dimension named above; an argument that names none is the same for every part. Nothing has to cross between parts.
Inputs may be any that keep to these rules, and one draw needn't show every extreme that they name: `qkv_image`: entries of standard deviation about 1/sqrt(3072). `qkv_text`: entries of standard deviation about 1/sqrt(3072).
All inputs are finite; a program needn't handle non-finite values.
Results may differ from the reference program's by a relative error of at most 0.0085.
Values may be sent and summed in bfloat16 or wider, within the bound.
A program may use at most 64 MiB of HBM per device.

```python
import jax
import jax.numpy as jnp
from jax import lax

D = 3072
HEADS = 16
HD = 128
STEPS = 50
IMAGE = 4096
TEXT = 512


def qkv_draw(key, salt):
    base = jax.random.truncated_normal(jax.random.fold_in(key, salt), -6.0, 6.0, (D, HEADS, 3, HD), jnp.float32) * float(D) ** (-0.5)
    return base.reshape(D, 3 * HEADS * HD)


def draw_qkv_image(key, part):
    return qkv_draw(key, 11).astype(jnp.bfloat16)


def draw_qkv_text(key, part):
    return qkv_draw(key, 13).astype(jnp.bfloat16)


def draw_norm_gain(key, part):
    logs = jax.random.uniform(jax.random.fold_in(key, 23), (2, 2, HEADS, HD), jnp.float32, jnp.log(1.2), jnp.log(3.0))
    result = jnp.exp(logs)
    return result.astype(jnp.float32)


def shard_levels(rng, shape, shards, low, high):
    loudness, own = 1.0, jax.random.fold_in(rng, 6)
    for axis_at, parts in shards:
        steps = jnp.exp(jax.random.uniform(jax.random.fold_in(own, axis_at), (parts,), jnp.float32, low / len(shards), high / len(shards)))
        loudness = loudness * jnp.repeat(steps, shape[axis_at] // parts).reshape([-1 if axis == axis_at else 1 for axis in range(len(shape))])
    return loudness


def normal_values(stream_key, extent, scale, reach, split=(), kind=jnp.bfloat16):
    values = scale * jax.random.normal(stream_key, extent, jnp.float32)
    if split:
        values = values * shard_levels(stream_key, extent, split, -0.22, 0.18)
    return jnp.clip(values, -reach, reach).astype(kind)


def setup_inputs(seed: int = 0, part: int = 0) -> dict:
    streams_of = jax.random.split(jax.random.key(seed), 12)
    part_keys = jax.random.split(jax.random.fold_in(streams_of[11], part), 12)
    return {
        "image_tokens": normal_values(part_keys[0], (IMAGE, D), 1.0, 6.0, ((0, 16),)),
        "text_tokens": normal_values(part_keys[1], (TEXT, D), 1.0, 6.0, ((0, 16),)),
        "timestep": jax.random.randint(part_keys[2], (1,), 0, STEPS).astype(jnp.int32),
        "text_length": jax.random.randint(part_keys[3], (1,), TEXT // 4, TEXT + 1).astype(jnp.int32),
        "time_table": normal_values(streams_of[4], (STEPS, D), 1.0, 6.0),
        "mod_weight": normal_values(streams_of[5], (D, 6 * D), D ** -0.5, 0.109375, ((0, 16), (1, 16))),
        "qkv_image": draw_qkv_image(jax.random.fold_in(streams_of[11], 71), part),
        "qkv_text": draw_qkv_text(jax.random.fold_in(streams_of[11], 71), part),
        "norm_gain": draw_norm_gain(jax.random.fold_in(streams_of[11], 71), part),
        "proj_image": normal_values(streams_of[9], (HEADS * HD, D), (HEADS * HD) ** -0.5, 0.125, ((0, 16), (1, 16))),
        "proj_text": normal_values(streams_of[10], (HEADS * HD, D), (HEADS * HD) ** -0.5, 0.125, ((0, 16), (1, 16))),
    }


EPSILON = 1e-06

def modulate(tokens, shift, scaling):
    values = tokens.astype(jnp.float32)
    center = lax.optimization_barrier(jnp.mean(values, axis=-1, keepdims=True))
    spread = lax.optimization_barrier(jnp.mean(jnp.square(values - center), axis=-1, keepdims=True))
    normed = (values - center) * lax.rsqrt(spread + EPSILON)
    return (normed * (1.0 + scaling) + shift).astype(jnp.bfloat16)

def head_norm(values, gain):
    return values * lax.rsqrt(lax.optimization_barrier(jnp.mean(values * values, axis=-1, keepdims=True)) + EPSILON) * gain

def split_heads(projected, gains):
    shaped = projected.reshape(projected.shape[0], -1, 3, gains.shape[-1])
    queries = head_norm(shaped[:, :, 0], gains[0]).astype(jnp.bfloat16)
    keys = head_norm(shaped[:, :, 1], gains[1]).astype(jnp.bfloat16)
    values = shaped[:, :, 2].astype(jnp.bfloat16)
    return (queries, keys, values)

def reference(image_tokens, text_tokens, timestep, text_length, time_table, mod_weight, qkv_image, qkv_text, norm_gain, proj_image, proj_text):
    embedded = lax.dynamic_index_in_dim(time_table, timestep[0], 0, keepdims=False).astype(jnp.float32)
    vector = jax.nn.silu(embedded).astype(jnp.bfloat16)
    modulation = jnp.dot(vector[None, :], mod_weight, preferred_element_type=jnp.float32)[0].reshape(2, 3, D)
    hidden_image = modulate(image_tokens, modulation[0, 0], modulation[0, 1])
    hidden_text = modulate(text_tokens, modulation[1, 0], modulation[1, 1])
    image_q, image_k, image_v = split_heads(jnp.dot(hidden_image, qkv_image, preferred_element_type=jnp.float32), norm_gain[0])
    text_q, text_k, text_v = split_heads(jnp.dot(hidden_text, qkv_text, preferred_element_type=jnp.float32), norm_gain[1])
    queries = jnp.concatenate([text_q, image_q], axis=0).transpose(1, 0, 2)
    keys = jnp.concatenate([text_k, image_k], axis=0).transpose(1, 0, 2)
    values = jnp.concatenate([text_v, image_v], axis=0).transpose(1, 0, 2)
    position = jnp.arange(TEXT + IMAGE, dtype=jnp.int32)
    usable = (position >= TEXT) | (position < text_length[0])
    factor = float(HD) ** (-0.5)

    def one_head(operands):
        head_q, head_k, head_v = operands
        scores = jnp.dot(head_q, head_k.T, preferred_element_type=jnp.float32) * factor
        scores = jnp.where(usable[None, :], scores, -1e+30)
        highest = lax.optimization_barrier(jnp.max(scores, axis=-1, keepdims=True))
        probs = jnp.exp(scores - highest)
        totals = lax.optimization_barrier(jnp.sum(probs, axis=-1, keepdims=True))
        mixed = jnp.dot(probs.astype(jnp.bfloat16), head_v, preferred_element_type=jnp.float32) / totals
        return mixed.astype(jnp.bfloat16)
    attended = lax.map(one_head, (queries, keys, values))
    attended = attended.transpose(1, 0, 2).reshape(TEXT + IMAGE, HEADS * HD)
    text_branch = jnp.dot(attended[:TEXT], proj_text, preferred_element_type=jnp.float32)
    image_branch = jnp.dot(attended[TEXT:], proj_image, preferred_element_type=jnp.float32)
    image_out = (image_tokens.astype(jnp.float32) + modulation[0, 2] * image_branch).astype(jnp.bfloat16)
    text_out = (text_tokens.astype(jnp.float32) + modulation[1, 2] * text_branch).astype(jnp.bfloat16)
    return (image_out, text_out)
```

```python
import functools
import math

import jax
import jax.numpy as jnp
from jax import lax
from jax.experimental import pallas as pl
from jax.experimental.pallas import tpu as pltpu
from jax.sharding import PartitionSpec as P

EPSILON = 1e-06
MESH = pl.DeviceIdType.MESH
BF16 = jnp.bfloat16
F32 = jnp.float32
RIGHT, LEFT = 0, 1


def rows_at(start, size, unit=16):
    if isinstance(start, int):
        return pl.ds(start, size)
    return pl.ds(pl.multiple_of(start, unit), size)


def cut_three(rows, unit, own):
    third = -(-rows // (3 * unit)) * unit
    rest = rows - 2 * third
    return (own * third, third), (2 * third, rest), ((1 - own) * third, third)


def kernel(
    sizes,
    paired,
    text_length,
    vector_rows,
    image_tokens,
    text_tokens,
    mod_weight,
    norm_gain,
    qkv_image,
    qkv_text,
    proj_image,
    proj_text,
    image_out,
    text_out,
    mod_z,
    mod_all,
    mean_of,
    rstd_of,
    hidden_image,
    hidden_text,
    weights,
    sum_image,
    sum_text,
    proj_z,
    proj_all,
    query,
    key_value,
    row_max,
    row_sum,
    mixed,
    attended,
    load_sem,
    modz_sems,
    modx_sems,
    w_sems,
    wy_sems,
    p_sems,
    py_sems,
    px_sems,
    kv_sems,
    ax_sems,
    as_sems,
):
    nz, nx, nc = sizes
    heads = nx * nc
    z = lax.axis_index("seq")
    x = lax.axis_index("tensor")
    c = lax.axis_index("sub")
    me = x * nc + c
    own = lax.rem(lax.axis_index("groups"), 2) if paired else 0
    other_group = lax.axis_index("groups") + 1 - 2 * own if paired else 0
    image_rows, width = image_tokens.shape
    text_rows = text_tokens.shape[0]
    local_rows = image_rows + text_rows
    slab = qkv_image.shape[0]
    columns = qkv_image.shape[1]
    size = columns // 3
    started = []

    def wrap(i, n):
        return lax.rem(i + n, n)

    def send(src, dst, sems, index, device):
        copy = pltpu.make_async_remote_copy(
            src_ref=src,
            dst_ref=dst,
            send_sem=sems.at[(0, *index)],
            recv_sem=sems.at[(1, *index)],
            device_id=device,
            device_id_type=MESH,
        )
        copy.start()
        started.append(copy)

    def arrive(ref, sems, index, device):
        pltpu.make_async_remote_copy(
            src_ref=ref,
            dst_ref=ref,
            send_sem=sems.at[(0, *index)],
            recv_sem=sems.at[(1, *index)],
            device_id=device,
            device_id_type=MESH,
        ).wait_recv()

    right, left = {"seq": wrap(z + 1, nz)}, {"seq": wrap(z - 1, nz)}
    partner = {"groups": other_group}
    sibling = {"sub": 1 - c}

    loads = [
        pltpu.make_async_copy(qkv_image, weights.at[z, :, pl.ds(0, columns)], load_sem.at[0]),
        pltpu.make_async_copy(qkv_text, weights.at[z, :, pl.ds(columns, columns)], load_sem.at[1]),
        pltpu.make_async_copy(proj_image, proj_z.at[z, 0], load_sem.at[2]),
        pltpu.make_async_copy(proj_text, proj_z.at[z, 1], load_sem.at[3]),
    ]
    for copy in loads:
        copy.start()

    barrier = pltpu.get_barrier_semaphore()
    peers = [{"seq": wrap(z + i, nz)} for i in range(1, nz)]
    plane = [
        {"tensor": lax.div(wrap(me + i, heads), nc), "sub": lax.rem(wrap(me + i, heads), nc)}
        for i in range(1, heads)
    ]
    greeted = peers + plane + ([partner] if paired else [])
    for device in greeted:
        pl.semaphore_signal(barrier, inc=1, device_id=device, device_id_type=MESH)

    mod_z[z] = jnp.dot(vector_rows[...], mod_weight[...], preferred_element_type=F32)

    chunk = 16

    def statistics(tokens, at):
        def one(i, carry):
            rows = rows_at(i * chunk, chunk)
            values = tokens[rows, :].astype(F32)
            center = jnp.mean(values, axis=-1, keepdims=True)
            spread = jnp.mean(jnp.square(values - center), axis=-1, keepdims=True)
            out = rows_at(at + i * chunk, chunk)
            mean_of[out, :] = jnp.broadcast_to(center, (chunk, 128))
            rstd_of[out, :] = jnp.broadcast_to(lax.rsqrt(spread + EPSILON), (chunk, 128))
            return carry

        lax.fori_loop(0, tokens.shape[0] // chunk, one, 0)

    for copy in loads:
        copy.wait()
    pl.semaphore_wait(barrier, len(greeted))

    for i in range(1, nz):
        send(mod_z.at[z], mod_z.at[z], modz_sems, (z,) if False else (i,), {"seq": wrap(z + i, nz)})

    half = nz // 2

    def slab_of(way, d):
        return wrap(z - d, nz) if way == RIGHT else wrap(z + d, nz)

    def parts_at(way, d):
        if d < half:
            return (0, 1)
        return (0,) if way == RIGHT else (1,)

    def ring_step(d, part_ref, sems):
        for way, to in ((RIGHT, right), (LEFT, left)):
            block = slab_of(way, d)
            for part in parts_at(way, d):
                if d > 0:
                    arrive(part_ref(block, part), sems, (way, d, part), to)
                if d < half and part in parts_at(way, d + 1):
                    send(part_ref(block, part), part_ref(block, part), sems, (way, d + 1, part), to)

    def pair_send(d, part_ref, sems):
        if not paired:
            return
        for way in (RIGHT, LEFT):
            if 0 in parts_at(way, d):
                block = slab_of(way, d)
                send(part_ref(block, 0), part_ref(block, 0), sems, (way, d), partner)

    def pair_wait(d, part_ref, sems):
        if not paired:
            return
        for way in (RIGHT, LEFT):
            if 0 in parts_at(way, d):
                arrive(part_ref(slab_of(way, d), 2), sems, (way, d), partner)

    if paired:
        w_parts = cut_three(slab, 16, own)
        p_parts = cut_three(size, 16, own)
    else:
        w_parts = ((0, slab // 2), (slab // 2, slab // 2))
        p_parts = ((0, size // 2), (size // 2, size // 2))

    def w_part(block, part):
        start, count = w_parts[part]
        return weights.at[block, rows_at(start, count), :]

    def p_part(block, part):
        start, count = p_parts[part]
        return proj_z.at[block, :, rows_at(start, count), :]

    ring_step(0, w_part, w_sems)

    statistics(text_tokens, 0)
    statistics(image_tokens, text_rows)

    def mod_over_seq():
        for i in range(1, nz):
            source = wrap(z - i, nz)
            arrive(mod_z.at[source], modz_sems, (i,), {"seq": source})
        total = mod_z[0]
        for i in range(1, nz):
            total = total + mod_z[i]
        mod_all[me] = total
        for i in range(1, heads):
            send(mod_all.at[me], mod_all.at[me], modx_sems, (i,), plane[i - 1])

    def mod_over_plane():
        for i in range(1, heads):
            source = wrap(me - i, heads)
            arrive(mod_all.at[source], modx_sems, (i,), plane[i - 1])

    piece = 2 * slab
    per_block = mod_weight.shape[1] // piece
    pieces = width // piece

    def mod_piece(index):
        if isinstance(index, int):
            return mod_all[index // per_block, :, pl.ds(index % per_block * piece, piece)]
        offset = pl.multiple_of(lax.rem(index, per_block) * piece, 128)
        return mod_all[lax.div(index, per_block), :, pl.ds(offset, piece)]

    def hide(tokens, hidden, stream, at):
        def one(i, carry):
            rows = rows_at(i * chunk, chunk)
            out = rows_at(at + i * chunk, chunk)
            center, scale = mean_of[out, 0:1], rstd_of[out, 0:1]
            for p in range(pieces):
                shift = mod_piece((stream * 3) * pieces + p)
                scaling = mod_piece((stream * 3 + 1) * pieces + p)
                values = tokens[rows, p * piece : (p + 1) * piece].astype(F32)
                values = ((values - center) * scale * (1.0 + scaling) + shift).astype(BF16)
                hidden[2 * p, rows, :] = values[:, :slab]
                hidden[2 * p + 1, rows, :] = values[:, slab:]
            return carry

        lax.fori_loop(0, tokens.shape[0] // chunk, one, 0)

    sum_image[...] = jnp.zeros_like(sum_image)
    sum_text[...] = jnp.zeros_like(sum_text)

    def project(first, last):
        def one(j, carry):
            step = lax.div(j + 1, 2)
            block = wrap(jnp.where(lax.rem(j, 2) == 1, z - step, z + step), nz)
            sum_image[...] += jnp.dot(
                hidden_image[block], weights[block, :, 0:columns], preferred_element_type=F32
            )
            sum_text[...] += jnp.dot(
                hidden_text[block],
                weights[block, :, columns : 2 * columns],
                preferred_element_type=F32,
            )
            return carry

        lax.fori_loop(first, last, one, 0)

    def give_block(block):
        to_x, to_c = lax.div(block, nc), lax.rem(block, nc)

        @pl.when(block != me)
        def _():
            pltpu.make_async_remote_copy(
                src_ref=proj_z.at[block],
                dst_ref=proj_all.at[me],
                send_sem=px_sems.at[0, block],
                recv_sem=px_sems.at[1, me],
                device_id={"tensor": to_x, "sub": to_c},
                device_id_type=MESH,
            ).start()

        @pl.when(block == me)
        def _():
            proj_all[me] = proj_z[block]

    def proj_step(d):
        ring_step(d, p_part, p_sems)
        pair_send(d, p_part, py_sems) if d > 0 else None
        if d > 1:
            proj_done(d - 1)
        if d == 0:
            give_block(z)

    def proj_done(d):
        pair_wait(d, p_part, py_sems)
        give_block(slab_of(RIGHT, d))
        if d < half:
            give_block(slab_of(LEFT, d))

    ready = min(3, half - 1)
    lag = min(5, half)
    done = 0
    for d in range(1, half + 1):
        ring_step(d, w_part, w_sems)
        pair_send(d, w_part, wy_sems)
        if d > 1:
            pair_wait(d - 1, w_part, wy_sems)
        if d >= lag:
            proj_step(d - lag)
        if d == 1:
            mod_over_seq()
        if d == ready:
            mod_over_plane()
            hide(text_tokens, hidden_text, 1, 0)
            hide(image_tokens, hidden_image, 0, text_rows)
        if d > ready:
            until = min(done + 4, 2 * d - 1)
            project(done, until)
            done = until
    proj_next = half - lag + 1
    pair_wait(half, w_part, wy_sems)
    project(done, nz)

    def normed(values, gain):
        return (
            values
            * lax.rsqrt(jnp.mean(values * values, axis=-1, keepdims=True) + EPSILON)
            * gain
        ).astype(BF16)

    for stream, total, at, count in (
        (1, sum_text, 0, text_rows),
        (0, sum_image, text_rows, image_rows),
    ):
        query[at : at + count, :] = normed(total[:, 0:size], norm_gain[stream, 0])
        key_value[z, at : at + count, 0:size] = normed(
            total[:, size : 2 * size], norm_gain[stream, 1]
        )
        key_value[z, at : at + count, size : 2 * size] = total[:, 2 * size : 3 * size].astype(BF16)

    half_rows = local_rows // 2

    def kv_part(block, part):
        return key_value.at[block, pl.ds(part * half_rows, half_rows), :]

    ring_step(0, kv_part, kv_sems)

    row_max[...] = jnp.full_like(row_max, -1e30)
    row_sum[...] = jnp.zeros_like(row_sum)
    mixed[...] = jnp.zeros_like(mixed)
    factor = float(size) ** (-0.5) * math.log2(math.e)

    def attend(first, last):
        def one(j, carry):
            step = lax.div(j + 1, 2)
            block = wrap(jnp.where(lax.rem(j, 2) == 1, z - step, z + step), nz)
            scores = lax.dot_general(
                query[...],
                key_value[block, :, 0:size],
                (((1,), (1,)), ((), ())),
                preferred_element_type=F32,
            )
            within = lax.broadcasted_iota(jnp.int32, scores.shape, 1)
            usable = (within >= text_rows) | (block * text_rows + within < text_length[0])
            scores = jnp.where(usable, scores, -1e30)
            old = row_max[:, 0:1]
            new = jnp.maximum(old, jnp.max(scores, axis=-1, keepdims=True))
            probs = jnp.exp2((scores - new) * factor)
            fade = jnp.exp2((old - new) * factor)
            row_max[...] = jnp.broadcast_to(new, row_max.shape)
            total = row_sum[:, 0:1] * fade + jnp.sum(probs, axis=-1, keepdims=True)
            row_sum[...] = jnp.broadcast_to(total, row_sum.shape)
            mixed[...] = mixed[...] * fade + jnp.dot(
                probs.astype(BF16),
                key_value[block, :, size : 2 * size],
                preferred_element_type=F32,
            )
            return carry

        lax.fori_loop(first, last, one, 0)

    attend(0, 1)
    for d in range(1, half + 1):
        ring_step(d, kv_part, kv_sems)
        if proj_next <= half:
            proj_step(proj_next)
            proj_next += 1
        attend(2 * d - 1, min(2 * d + 1, nz))
    while proj_next <= half:
        proj_step(proj_next)
        proj_next += 1

    attended[me] = (mixed[...] / row_sum[:, 0:1]).astype(BF16)
    proj_done(half)

    x_half = nx // 2
    x_right, x_left = {"tensor": wrap(x + 1, nx)}, {"tensor": wrap(x - 1, nx)}

    def x_parts(way, d):
        if d < x_half:
            return (0, 1)
        return (0,) if way == RIGHT else (1,)

    def x_block(way, d):
        return (wrap(x - d, nx) if way == RIGHT else wrap(x + d, nx)) * nc + c

    def a_part(block, part):
        return attended.at[block, pl.ds(part * half_rows, half_rows), :]

    for part in (0, 1):
        for way, to in ((RIGHT, x_right), (LEFT, x_left)):
            if part in x_parts(way, 1):
                send(a_part(me, part), a_part(me, part), ax_sems, (way, 1, part), to)
        send(a_part(me, part), a_part(me, part), as_sems, (RIGHT, 0, part), sibling)
    for d in range(1, x_half + 1):
        for part in (0, 1):
            for way, to in ((RIGHT, x_right), (LEFT, x_left)):
                if part not in x_parts(way, d):
                    continue
                block = x_block(way, d)
                arrive(a_part(block, part), ax_sems, (way, d, part), to)
                if d < x_half and part in x_parts(way, d + 1):
                    send(a_part(block, part), a_part(block, part), ax_sems, (way, d + 1, part), to)
                send(a_part(block, part), a_part(block, part), as_sems, (way, d, part), sibling)

    for i in range(1, heads):
        source = wrap(me + i, heads)
        pltpu.make_async_remote_copy(
            src_ref=proj_all.at[source],
            dst_ref=proj_all.at[source],
            send_sem=px_sems.at[0, source],
            recv_sem=px_sems.at[1, source],
            device_id=sibling,
            device_id_type=MESH,
        ).wait_recv()

    across = 1 - 2 * c
    for d in range(0, x_half + 1):
        for part in (0, 1):
            for way in (RIGHT, LEFT):
                if d == 0 and way == LEFT:
                    continue
                if d > 0 and part not in x_parts(way, d):
                    continue
                block = (me if d == 0 else x_block(way, d)) + across
                arrive(a_part(block, part), as_sems, (way, d, part), sibling)

    out_width = image_out.shape[1]
    sum_out = None
    image_sum, text_sum = None, None
    for h in range(0, heads, 2):
        rows = jnp.concatenate([attended[h], attended[h + 1]], axis=1)
        image_w = jnp.concatenate([proj_all[h, 0], proj_all[h + 1, 0]], axis=0)
        text_w = jnp.concatenate([proj_all[h, 1], proj_all[h + 1, 1]], axis=0)
        image_term = jnp.dot(rows[text_rows:], image_w, preferred_element_type=F32)
        text_term = jnp.dot(rows[:text_rows], text_w, preferred_element_type=F32)
        image_sum = image_term if image_sum is None else image_sum + image_term
        text_sum = text_term if text_sum is None else text_sum + text_term

    def own_columns(wide):
        return jnp.where(c == 0, wide[:, :out_width], wide[:, out_width:])

    window = pl.ds(pl.multiple_of(x * 2 * out_width, 128), 2 * out_width)
    for tokens, total, out, stream in (
        (image_tokens, image_sum, image_out, 0),
        (text_tokens, text_sum, text_out, 1),
    ):
        gate = own_columns(mod_piece((stream * 3 + 2) * pieces + x))
        base = own_columns(tokens[:, window].astype(F32))
        out[...] = (base + gate * total).astype(BF16)

    for copy in started:
        copy.wait_send()
    for i in range(1, heads):
        block = wrap(me + i, heads)
        pltpu.make_async_remote_copy(
            src_ref=proj_z.at[block],
            dst_ref=proj_all.at[me],
            send_sem=px_sems.at[0, block],
            recv_sem=px_sems.at[1, me],
            device_id=sibling,
            device_id_type=MESH,
        ).wait_send()


def solution(mesh):
    nz, nx, nc = mesh.shape["seq"], mesh.shape["tensor"], mesh.shape["sub"]
    paired = mesh.shape["groups"] % 2 == 0
    heads = nx * nc

    def body(
        image_tokens,
        text_tokens,
        timestep,
        text_length,
        time_table,
        mod_weight,
        qkv_image,
        qkv_text,
        norm_gain,
        proj_image,
        proj_text,
    ):
        slab = qkv_image.shape[0]
        embedded = lax.dynamic_slice(
            time_table, (timestep[0], lax.axis_index("seq") * slab), (1, slab)
        ).astype(F32)
        vector_rows = jax.nn.silu(embedded).astype(BF16)
        gains = norm_gain.reshape(2, 2, 1, norm_gain.shape[-1])
        image_rows, width = image_tokens.shape
        text_rows = text_tokens.shape[0]
        local_rows = image_rows + text_rows
        columns = qkv_image.shape[1]
        size = columns // 3
        out_width = width // heads
        half = nz // 2
        vmem = pl.BlockSpec(memory_space=pltpu.VMEM)
        anywhere = pl.BlockSpec(memory_space=pl.ANY)
        dma = pltpu.SemaphoreType.DMA
        return pl.pallas_call(
            functools.partial(kernel, (nz, nx, nc), paired),
            out_shape=(
                jax.ShapeDtypeStruct((image_rows, out_width), BF16),
                jax.ShapeDtypeStruct((text_rows, out_width), BF16),
            ),
            in_specs=[pl.BlockSpec(memory_space=pltpu.SMEM)] + [vmem] * 5 + [anywhere] * 4,
            out_specs=(vmem, vmem),
            scratch_shapes=[
                pltpu.VMEM((nz, 1, mod_weight.shape[1]), F32),
                pltpu.VMEM((heads, 1, mod_weight.shape[1]), F32),
                pltpu.VMEM((local_rows, 128), F32),
                pltpu.VMEM((local_rows, 128), F32),
                pltpu.VMEM((nz, image_rows, slab), BF16),
                pltpu.VMEM((nz, text_rows, slab), BF16),
                pltpu.VMEM((nz, slab, 2 * columns), BF16),
                pltpu.VMEM((image_rows, columns), F32),
                pltpu.VMEM((text_rows, columns), F32),
                pltpu.VMEM((nz, 2, *proj_image.shape), BF16),
                pltpu.VMEM((heads, 2, *proj_image.shape), BF16),
                pltpu.VMEM((local_rows, size), BF16),
                pltpu.VMEM((nz, local_rows, 2 * size), BF16),
                pltpu.VMEM((local_rows, 128), F32),
                pltpu.VMEM((local_rows, 128), F32),
                pltpu.VMEM((local_rows, size), F32),
                pltpu.VMEM((heads, local_rows, size), BF16),
                dma((4,)),
                dma((2, nz)),
                dma((2, heads)),
                dma((2, 2, half + 1, 2)),
                dma((2, 2, half + 1)),
                dma((2, 2, half + 1, 2)),
                dma((2, 2, half + 1)),
                dma((2, heads)),
                dma((2, 2, half + 1, 2)),
                dma((2, 2, nx // 2 + 1, 2)),
                dma((2, 2, nx // 2 + 1, 2)),
            ],
            compiler_params=pltpu.CompilerParams(
                collective_id=0, has_side_effects=True, vmem_limit_bytes=56 * 1024 * 1024
            ),
        )(
            text_length,
            vector_rows,
            image_tokens,
            text_tokens,
            mod_weight,
            gains,
            qkv_image,
            qkv_text,
            proj_image,
            proj_text,
        )

    return jax.shard_map(
        body,
        mesh=mesh,
        in_specs=(
            P(("groups", "seq"), None),
            P(("groups", "seq"), None),
            P("groups"),
            P("groups"),
            P(),
            P("seq", ("tensor", "sub")),
            P("seq", ("tensor", "sub")),
            P("seq", ("tensor", "sub")),
            P(None, None, ("tensor", "sub"), None),
            P(("tensor", "sub"), "seq"),
            P(("tensor", "sub"), "seq"),
        ),
        out_specs=(
            P(("groups", "seq"), ("tensor", "sub")),
            P(("groups", "seq"), ("tensor", "sub")),
        ),
        check_vma=False,
    )
```

```python
import functools
import math

import jax
import jax.numpy as jnp
from jax import lax
from jax.experimental import pallas as pl
from jax.experimental.pallas import tpu as pltpu
from jax.sharding import PartitionSpec as P

EPSILON = 1e-06
MESH = pl.DeviceIdType.MESH
BF16 = jnp.bfloat16
F32 = jnp.float32
RIGHT, LEFT = 0, 1


def rows_at(start, size, unit=16):
    if isinstance(start, int):
        return pl.ds(start, size)
    return pl.ds(pl.multiple_of(start, unit), size)


def cut_three(rows, own):
    alone = -(-rows * 5 // (12 * 16)) * 16
    return (own * alone, alone), (2 * alone, rows - 2 * alone), ((1 - own) * alone, alone)


def kernel(
    sizes,
    paired,
    text_length,
    timestep,
    image_hbm,
    text_hbm,
    table_hbm,
    mod_hbm,
    gain_hbm,
    qkv_image,
    qkv_text,
    proj_image,
    proj_text,
    image_out,
    text_out,
    image_tokens,
    text_tokens,
    time_table,
    mod_weight,
    norm_gain,
    mod_z,
    mod_all,
    mean_of,
    rstd_of,
    hidden_image,
    hidden_text,
    weights,
    text_weights,
    sum_image,
    sum_text,
    text_qkv,
    proj_z,
    proj_all,
    query,
    key_value,
    row_max,
    row_sum,
    mixed,
    attended,
    load_sem,
    modz_sems,
    modx_sems,
    w_sems,
    wy_sems,
    t_sems,
    th_sems,
    tq_sems,
    p_sems,
    py_sems,
    px_sems,
    kv_sems,
    ax_sems,
    as_sems,
):
    nz, nx, nc = sizes
    heads = nx * nc
    z = lax.axis_index("seq")
    x = lax.axis_index("tensor")
    c = lax.axis_index("sub")
    me = x * nc + c
    own = lax.rem(lax.axis_index("groups"), 2) if paired else 0
    other_group = lax.axis_index("groups") + 1 - 2 * own if paired else 0
    image_rows, width = image_tokens.shape
    text_rows = text_tokens.shape[0]
    local_rows = image_rows + text_rows
    slab = qkv_image.shape[0]
    columns = qkv_image.shape[1]
    size = columns // 3
    started = []
    active = c == own

    def when_active(run):
        if paired:
            pl.when(active)(run)
        else:
            run()


    def wrap(i, n):
        return lax.rem(i + n, n)

    def send(src, dst, sems, index, device, keep=True):
        copy = pltpu.make_async_remote_copy(
            src_ref=src,
            dst_ref=dst,
            send_sem=sems.at[(0, *index)],
            recv_sem=sems.at[(1, *index)],
            device_id=device,
            device_id_type=MESH,
        )
        copy.start()
        if keep:
            started.append(copy)

    def arrive(ref, sems, index, device):
        pltpu.make_async_remote_copy(
            src_ref=ref,
            dst_ref=ref,
            send_sem=sems.at[(0, *index)],
            recv_sem=sems.at[(1, *index)],
            device_id=device,
            device_id_type=MESH,
        ).wait_recv()

    right, left = {"seq": wrap(z + 1, nz)}, {"seq": wrap(z - 1, nz)}
    partner = {"groups": other_group}
    sibling = {"sub": 1 - c}

    barrier = pltpu.get_barrier_semaphore()
    peers = [{"seq": wrap(z + i, nz)} for i in range(1, nz)]
    plane = [
        {"tensor": lax.div(wrap(me + i, heads), nc), "sub": lax.rem(wrap(me + i, heads), nc)}
        for i in range(1, heads)
    ]
    greeted = peers + plane + ([partner] if paired else [])
    for device in greeted:
        pl.semaphore_signal(barrier, inc=1, device_id=device, device_id_type=MESH)

    piece = 2 * slab
    table_window = pl.ds(pl.multiple_of(lax.div(z, 2) * piece, 128), piece)
    loads = [
        pltpu.make_async_copy(src, dst, load_sem.at[i])
        for i, (src, dst) in enumerate(
            (
                (table_hbm.at[:, table_window], time_table),
                (mod_hbm, mod_weight),
                (qkv_image, weights.at[z]),
                (qkv_text, text_weights.at[z]),
                (proj_image, proj_z.at[z, 0]),
                (proj_text, proj_z.at[z, 1]),
                (text_hbm, text_tokens),
                (image_hbm, image_tokens),
                (gain_hbm, norm_gain),
            )
        )
    ]
    for copy in loads:
        copy.start()
    for copy in loads[:6]:
        copy.wait()

    picked = lax.broadcasted_iota(jnp.int32, time_table.shape, 0) == timestep[0]
    embedded = jnp.sum(
        jnp.where(picked, time_table[...].astype(F32), 0.0), axis=0, keepdims=True
    )
    vector = (embedded / (1.0 + jnp.exp(-embedded))).astype(BF16)
    vector_rows = jnp.where(lax.rem(z, 2) == 0, vector[:, :slab], vector[:, slab:])
    mod_z[z] = jnp.dot(vector_rows, mod_weight[...], preferred_element_type=F32)

    chunk = 16

    def statistics(tokens, at):
        def one(i, carry):
            rows = rows_at(i * chunk, chunk)
            values = tokens[rows, :].astype(F32)
            center = jnp.mean(values, axis=-1, keepdims=True)
            spread = jnp.mean(jnp.square(values - center), axis=-1, keepdims=True)
            out = rows_at(at + i * chunk, chunk)
            mean_of[out, :] = jnp.broadcast_to(center, (chunk, 128))
            rstd_of[out, :] = jnp.broadcast_to(lax.rsqrt(spread + EPSILON), (chunk, 128))
            return carry

        lax.fori_loop(0, tokens.shape[0] // chunk, one, 0)

    pl.semaphore_wait(barrier, len(greeted))

    for i in range(1, nz):
        send(mod_z.at[z], mod_z.at[z], modz_sems, (i,), peers[i - 1])

    half = nz // 2

    def slab_of(way, d):
        return wrap(z - d, nz) if way == RIGHT else wrap(z + d, nz)

    def parts_at(way, d):
        if d < half:
            return (0, 1)
        return (0,) if way == RIGHT else (1,)

    def ring_step(d, part_ref, sems, keep=True):
        for way, to in ((RIGHT, right), (LEFT, left)):
            block = slab_of(way, d)
            for part in parts_at(way, d):
                if d > 0:
                    arrive(part_ref(block, part), sems, (way, d, part), to)
                if d < half and part in parts_at(way, d + 1):
                    here = part_ref(block, part)
                    send(here, here, sems, (way, d + 1, part), to, keep)

    def pair_send(d, part_ref, sems):
        if not paired:
            return
        for way in (RIGHT, LEFT):
            if 0 in parts_at(way, d):
                block = slab_of(way, d)
                send(part_ref(block, 0), part_ref(block, 0), sems, (way, d), partner)

    def pair_wait(d, part_ref, sems):
        if not paired:
            return
        for way in (RIGHT, LEFT):
            if 0 in parts_at(way, d):
                arrive(part_ref(slab_of(way, d), 2), sems, (way, d), partner)

    if paired:
        w_parts = cut_three(slab, own)
    else:
        w_parts = ((0, slab // 2), (slab // 2, slab // 2))

    def w_part(block, part):
        start, count = w_parts[part]
        return weights.at[block, rows_at(start, count), :]

    def t_part(block, part):
        return text_weights.at[block, pl.ds(part * (slab // 2), slab // 2), :]

    def p_part(block, part):
        start, count = w_parts[part]
        return proj_z.at[block, :, rows_at(start, count), :]

    def text_step(d):
        when_active(lambda: ring_step(d, t_part, t_sems, False))

    ring_step(0, w_part, w_sems)
    text_step(0)
    ring_step(0, p_part, p_sems)

    for copy in loads[6:]:
        copy.wait()
    statistics(text_tokens, image_rows)
    statistics(image_tokens, 0)

    def mod_over_seq():
        for i in range(1, nz):
            source = wrap(z - i, nz)
            arrive(mod_z.at[source], modz_sems, (i,), {"seq": source})
        total = mod_z[0]
        for i in range(1, nz):
            total = total + mod_z[i]
        mod_all[me] = total
        for i in range(1, heads):
            send(mod_all.at[me], mod_all.at[me], modx_sems, (i,), plane[i - 1])

    def mod_over_plane():
        for i in range(1, heads):
            source = wrap(me - i, heads)
            arrive(mod_all.at[source], modx_sems, (i,), plane[i - 1])

    per_block = mod_weight.shape[1] // piece
    pieces = width // piece

    def mod_piece(index):
        if isinstance(index, int):
            return mod_all[index // per_block, :, pl.ds(index % per_block * piece, piece)]
        offset = pl.multiple_of(lax.rem(index, per_block) * piece, 128)
        return mod_all[lax.div(index, per_block), :, pl.ds(offset, piece)]

    def hide(tokens, hidden, stream, at):
        def one(i, carry):
            rows = rows_at(i * chunk, chunk)
            out = rows_at(at + i * chunk, chunk)
            center, scale = mean_of[out, 0:1], rstd_of[out, 0:1]
            for p in range(pieces):
                shift = mod_piece((stream * 3) * pieces + p)
                scaling = mod_piece((stream * 3 + 1) * pieces + p)
                values = tokens[rows, p * piece : (p + 1) * piece].astype(F32)
                values = ((values - center) * scale * (1.0 + scaling) + shift).astype(BF16)
                hidden[2 * p, rows, :] = values[:, :slab]
                hidden[2 * p + 1, rows, :] = values[:, slab:]
            return carry

        lax.fori_loop(0, tokens.shape[0] // chunk, one, 0)

    sum_image[...] = jnp.zeros_like(sum_image)
    sum_text[...] = jnp.zeros_like(sum_text)

    def block_at(j):
        step = lax.div(j + 1, 2)
        return wrap(jnp.where(lax.rem(j, 2) == 1, z - step, z + step), nz)

    def project(hidden, total, shards, first, last):
        def one(j, carry):
            block = block_at(j)
            total[...] += jnp.dot(hidden[block], shards[block], preferred_element_type=F32)
            return carry

        lax.fori_loop(first, last, one, 0)

    def give_block(block):
        to_x, to_c = lax.div(block, nc), lax.rem(block, nc)

        @pl.when(block != me)
        def _():
            pltpu.make_async_remote_copy(
                src_ref=proj_z.at[block],
                dst_ref=proj_all.at[me],
                send_sem=px_sems.at[0, block],
                recv_sem=px_sems.at[1, me],
                device_id={"tensor": to_x, "sub": to_c},
                device_id_type=MESH,
            ).start()

        @pl.when(block == me)
        def _():
            proj_all[me] = proj_z[block]

    def proj_done(d):
        pair_wait(d, p_part, py_sems)
        give_block(slab_of(RIGHT, d))
        if 0 < d < half:
            give_block(slab_of(LEFT, d))

    give_block(z)
    ready = min(3, half - 1)
    done = 0
    both = hidden_text.at[:, pl.ds(0, text_rows), :], hidden_text.at[:, pl.ds(text_rows, text_rows), :]
    for d in range(1, half + 1):
        ring_step(d, w_part, w_sems)
        text_step(d)
        pair_send(d, w_part, wy_sems)
        ring_step(d, p_part, p_sems)
        pair_send(d, p_part, py_sems)
        if d == 1:
            mod_over_seq()
        if d == ready:
            mod_over_plane()
            hide(text_tokens, hidden_text, 1, image_rows)
            if paired:

                @pl.when(jnp.logical_not(active))
                def _():
                    send(both[0], both[1], th_sems, (), partner, False)

            hide(image_tokens, hidden_image, 0, 0)
        if d > 1:
            pair_wait(d - 1, w_part, wy_sems)
            proj_done(d - 1)
        if d > ready:
            until = min(done + 4, 2 * d - 1)
            project(hidden_image, sum_image, weights, done, until)
            done = until
    pair_wait(half, w_part, wy_sems)
    project(hidden_image, sum_image, weights, done, nz)

    def normed(values, gain):
        return (
            values
            * lax.rsqrt(jnp.mean(values * values, axis=-1, keepdims=True) + EPSILON)
            * gain
        ).astype(BF16)

    def normed_three(total, stream):
        return (
            normed(total[:, 0:size], norm_gain[stream, 0]),
            normed(total[:, size : 2 * size], norm_gain[stream, 1]),
            total[:, 2 * size : 3 * size].astype(BF16),
        )

    half_rows = local_rows // 2

    def kv_part(block, part):
        return key_value.at[block, pl.ds(part * half_rows, half_rows), :]

    def kv_send(part):
        for way, to in ((RIGHT, right), (LEFT, left)):
            if part in parts_at(way, 1):
                send(kv_part(z, part), kv_part(z, part), kv_sems, (way, 1, part), to)

    q, k, v = normed_three(sum_image[...], 0)
    query[0:image_rows, :] = q
    key_value[z, 0:image_rows, 0:size] = k
    key_value[z, 0:image_rows, size : 2 * size] = v
    kv_send(0)

    def text_projection():
        if paired:
            arrive(both[1], th_sems, (), partner)
        project(hidden_text, sum_text, text_weights, 0, nz)
        for side in (0, 1) if paired else (0,):
            parts = normed_three(sum_text[side * text_rows : (side + 1) * text_rows, :], 1)
            for i in range(3):
                text_qkv[side, :, i * size : (i + 1) * size] = parts[i]
        if paired:
            send(text_qkv.at[1], text_qkv.at[0], tq_sems, (), partner, False)

    when_active(text_projection)
    if paired:

        @pl.when(jnp.logical_not(active))
        def _():
            arrive(text_qkv.at[0], tq_sems, (), partner)

    query[image_rows:, :] = text_qkv[0, :, 0:size]
    key_value[z, image_rows:, :] = text_qkv[0, :, size : 3 * size]
    kv_send(1)
    proj_done(half)

    row_max[...] = jnp.full_like(row_max, -1e30)
    row_sum[...] = jnp.zeros_like(row_sum)
    mixed[...] = jnp.zeros_like(mixed)
    factor = float(size) ** (-0.5) * math.log2(math.e)

    def attend(first, last):
        def one(j, carry):
            block = block_at(j)
            scores = lax.dot_general(
                query[...],
                key_value[block, :, 0:size],
                (((1,), (1,)), ((), ())),
                preferred_element_type=F32,
            )
            within = lax.broadcasted_iota(jnp.int32, scores.shape, 1)
            slot = block * text_rows + within - image_rows
            usable = (within < image_rows) | (slot < text_length[0])
            scores = jnp.where(usable, scores, -1e30)
            old = row_max[:, 0:1]
            new = jnp.maximum(old, jnp.max(scores, axis=-1, keepdims=True))
            probs = jnp.exp2((scores - new) * factor)
            fade = jnp.exp2((old - new) * factor)
            row_max[...] = jnp.broadcast_to(new, row_max.shape)
            total = row_sum[:, 0:1] * fade + jnp.sum(probs, axis=-1, keepdims=True)
            row_sum[...] = jnp.broadcast_to(total, row_sum.shape)
            mixed[...] = mixed[...] * fade + jnp.dot(
                probs.astype(BF16),
                key_value[block, :, size : 2 * size],
                preferred_element_type=F32,
            )
            return carry

        lax.fori_loop(first, last, one, 0)

    attend(0, 1)
    for d in range(1, half + 1):
        ring_step(d, kv_part, kv_sems)
        attend(2 * d - 1, min(2 * d + 1, nz))

    attended[me] = (mixed[...] / row_sum[:, 0:1]).astype(BF16)

    x_half = nx // 2
    x_right, x_left = {"tensor": wrap(x + 1, nx)}, {"tensor": wrap(x - 1, nx)}

    def x_parts(way, d):
        if d < x_half:
            return (0, 1)
        return (0,) if way == RIGHT else (1,)

    def x_block(way, d):
        return (wrap(x - d, nx) if way == RIGHT else wrap(x + d, nx)) * nc + c

    def a_part(block, part):
        return attended.at[block, pl.ds(part * half_rows, half_rows), :]

    for part in (0, 1):
        for way, to in ((RIGHT, x_right), (LEFT, x_left)):
            if part in x_parts(way, 1):
                send(a_part(me, part), a_part(me, part), ax_sems, (way, 1, part), to)
        send(a_part(me, part), a_part(me, part), as_sems, (RIGHT, 0, part), sibling)
    for d in range(1, x_half + 1):
        for part in (0, 1):
            for way, to in ((RIGHT, x_right), (LEFT, x_left)):
                if part not in x_parts(way, d):
                    continue
                block = x_block(way, d)
                arrive(a_part(block, part), ax_sems, (way, d, part), to)
                if d < x_half and part in x_parts(way, d + 1):
                    send(a_part(block, part), a_part(block, part), ax_sems, (way, d + 1, part), to)
                send(a_part(block, part), a_part(block, part), as_sems, (way, d, part), sibling)

    for i in range(1, heads):
        source = wrap(me + i, heads)
        pltpu.make_async_remote_copy(
            src_ref=proj_all.at[source],
            dst_ref=proj_all.at[source],
            send_sem=px_sems.at[0, source],
            recv_sem=px_sems.at[1, source],
            device_id=sibling,
            device_id_type=MESH,
        ).wait_recv()

    across = 1 - 2 * c
    for d in range(0, x_half + 1):
        for part in (0, 1):
            for way in (RIGHT, LEFT):
                if d == 0 and way == LEFT:
                    continue
                if d > 0 and part not in x_parts(way, d):
                    continue
                block = (me if d == 0 else x_block(way, d)) + across
                arrive(a_part(block, part), as_sems, (way, d, part), sibling)

    out_width = image_out.shape[1]
    image_sum, text_sum = None, None
    for h in range(0, heads, 2):
        rows = jnp.concatenate([attended[h], attended[h + 1]], axis=1)
        image_w = jnp.concatenate([proj_all[h, 0], proj_all[h + 1, 0]], axis=1)
        text_w = jnp.concatenate([proj_all[h, 1], proj_all[h + 1, 1]], axis=1)
        turned = (((1,), (1,)), ((), ()))
        image_term = lax.dot_general(
            rows[:image_rows], image_w, turned, preferred_element_type=F32
        )
        text_term = lax.dot_general(rows[image_rows:], text_w, turned, preferred_element_type=F32)
        image_sum = image_term if image_sum is None else image_sum + image_term
        text_sum = text_term if text_sum is None else text_sum + text_term

    def own_columns(wide):
        return jnp.where(c == 0, wide[:, :out_width], wide[:, out_width:])

    window = pl.ds(pl.multiple_of(x * 2 * out_width, 128), 2 * out_width)
    for tokens, total, out, stream in (
        (image_tokens, image_sum, image_out, 0),
        (text_tokens, text_sum, text_out, 1),
    ):
        gate = own_columns(mod_piece((stream * 3 + 2) * pieces + x))
        base = own_columns(tokens[:, window].astype(F32))
        out[...] = (base + gate * total).astype(BF16)

    for copy in started:
        copy.wait_send()

    def sent(ref, sems, index, device):
        pltpu.make_async_remote_copy(
            src_ref=ref,
            dst_ref=ref,
            send_sem=sems.at[(0, *index)],
            recv_sem=sems.at[(1, *index)],
            device_id=device,
            device_id_type=MESH,
        ).wait_send()

    def text_sent():
        for d in range(1, half + 1):
            for way, to in ((RIGHT, right), (LEFT, left)):
                for part in parts_at(way, d):
                    sent(t_part(z, part), t_sems, (way, d, part), to)
        if paired:
            sent(text_qkv.at[1], tq_sems, (), partner)

    when_active(text_sent)
    if paired:

        @pl.when(jnp.logical_not(active))
        def _():
            sent(both[0], th_sems, (), partner)

    for i in range(1, heads):
        block = wrap(me + i, heads)
        pltpu.make_async_remote_copy(
            src_ref=proj_z.at[block],
            dst_ref=proj_all.at[me],
            send_sem=px_sems.at[0, block],
            recv_sem=px_sems.at[1, me],
            device_id=sibling,
            device_id_type=MESH,
        ).wait_send()


def solution(mesh):
    nz, nx, nc = mesh.shape["seq"], mesh.shape["tensor"], mesh.shape["sub"]
    paired = mesh.shape["groups"] % 2 == 0
    heads = nx * nc

    def body(
        image_tokens,
        text_tokens,
        timestep,
        text_length,
        time_table,
        mod_weight,
        qkv_image,
        qkv_text,
        norm_gain,
        proj_image,
        proj_text,
    ):
        slab = qkv_image.shape[0]
        gains = norm_gain.reshape(2, 2, 1, norm_gain.shape[-1])
        image_rows, width = image_tokens.shape
        text_rows = text_tokens.shape[0]
        local_rows = image_rows + text_rows
        columns = qkv_image.shape[1]
        size = columns // 3
        out_width = width // heads
        half = nz // 2
        vmem = pl.BlockSpec(memory_space=pltpu.VMEM)
        anywhere = pl.BlockSpec(memory_space=pl.ANY)
        dma = pltpu.SemaphoreType.DMA
        return pl.pallas_call(
            functools.partial(kernel, (nz, nx, nc), paired),
            out_shape=(
                jax.ShapeDtypeStruct((image_rows, out_width), BF16),
                jax.ShapeDtypeStruct((text_rows, out_width), BF16),
            ),
            in_specs=[pl.BlockSpec(memory_space=pltpu.SMEM)] * 2 + [anywhere] * 9,
            out_specs=(vmem, vmem),
            scratch_shapes=[
                pltpu.VMEM(image_tokens.shape, BF16),
                pltpu.VMEM(text_tokens.shape, BF16),
                pltpu.VMEM((time_table.shape[0], 2 * slab), BF16),
                pltpu.VMEM(mod_weight.shape, BF16),
                pltpu.VMEM(gains.shape, F32),
                pltpu.VMEM((nz, 1, mod_weight.shape[1]), F32),
                pltpu.VMEM((heads, 1, mod_weight.shape[1]), F32),
                pltpu.VMEM((local_rows, 128), F32),
                pltpu.VMEM((local_rows, 128), F32),
                pltpu.VMEM((nz, image_rows, slab), BF16),
                pltpu.VMEM((nz, 2 * text_rows, slab), BF16),
                pltpu.VMEM((nz, slab, columns), BF16),
                pltpu.VMEM((nz, slab, columns), BF16),
                pltpu.VMEM((image_rows, columns), F32),
                pltpu.VMEM((2 * text_rows, columns), F32),
                pltpu.VMEM((2, text_rows, columns), BF16),
                pltpu.VMEM((nz, 2, *proj_image.shape[::-1]), BF16),
                pltpu.VMEM((heads, 2, *proj_image.shape[::-1]), BF16),
                pltpu.VMEM((local_rows, size), BF16),
                pltpu.VMEM((nz, local_rows, 2 * size), BF16),
                pltpu.VMEM((local_rows, 128), F32),
                pltpu.VMEM((local_rows, 128), F32),
                pltpu.VMEM((local_rows, size), F32),
                pltpu.VMEM((heads, local_rows, size), BF16),
                dma((9,)),
                dma((2, nz)),
                dma((2, heads)),
                dma((2, 2, half + 1, 2)),
                dma((2, 2, half + 1)),
                dma((2, 2, half + 1, 2)),
                dma((2,)),
                dma((2,)),
                dma((2, 2, half + 1, 2)),
                dma((2, 2, half + 1)),
                dma((2, heads)),
                dma((2, 2, half + 1, 2)),
                dma((2, 2, nx // 2 + 1, 2)),
                dma((2, 2, nx // 2 + 1, 2)),
            ],
            compiler_params=pltpu.CompilerParams(
                collective_id=0, has_side_effects=True, vmem_limit_bytes=56 * 1024 * 1024
            ),
        )(
            text_length,
            timestep,
            image_tokens,
            text_tokens,
            time_table,
            mod_weight,
            gains,
            qkv_image,
            qkv_text,
            proj_image.T,
            proj_text.T,
        )

    return jax.shard_map(
        body,
        mesh=mesh,
        in_specs=(
            P(("groups", "seq"), None),
            P(("groups", "seq"), None),
            P("groups"),
            P("groups"),
            P(),
            P("seq", ("tensor", "sub")),
            P("seq", ("tensor", "sub")),
            P("seq", ("tensor", "sub")),
            P(None, None, ("tensor", "sub"), None),
            P(("tensor", "sub"), "seq"),
            P(("tensor", "sub"), "seq"),
        ),
        out_specs=(
            P(("groups", "seq"), ("tensor", "sub")),
            P(("groups", "seq"), ("tensor", "sub")),
        ),
        check_vma=False,
    )
```

```python
import functools
import math

import jax
import jax.numpy as jnp
from jax import lax
from jax.experimental import pallas as pl
from jax.experimental.pallas import tpu as pltpu
from jax.sharding import PartitionSpec as P

EPSILON = 1e-06
MESH = pl.DeviceIdType.MESH
BF16 = jnp.bfloat16
F32 = jnp.float32
RIGHT, LEFT = 0, 1


def rows_at(start, size, unit=16):
    if isinstance(start, int):
        return pl.ds(start, size)
    return pl.ds(pl.multiple_of(start, unit), size)


def kernel(
    sizes,
    paired,
    text_length,
    timestep,
    image_hbm,
    text_hbm,
    table_hbm,
    mod_hbm,
    gain_hbm,
    qkv_image,
    qkv_text,
    proj_image,
    proj_text,
    image_out,
    text_out,
    image_tokens,
    text_tokens,
    time_table,
    mod_weight,
    norm_gain,
    mod_z,
    mod_all,
    mean_of,
    rstd_of,
    hidden_image,
    hidden_text,
    weights,
    text_weights,
    sum_image,
    sum_text,
    text_qkv,
    proj_z,
    proj_all,
    query,
    key_value,
    row_max,
    row_sum,
    mixed,
    attended,
    load_sem,
    *pairs,
):
    nz, nx, nc = sizes
    (
        modz_sems,
        modx_sems,
        w_sems,
        wy_sems,
        t_sems,
        th_sems,
        tq_sems,
        p_sems,
        py_sems,
        px_sems,
        kv_sems,
        ax_sems,
        as_sems,
    ) = zip(pairs[0::2], pairs[1::2])
    heads = nx * nc
    z = lax.axis_index("seq")
    x = lax.axis_index("tensor")
    c = lax.axis_index("sub")
    me = x * nc + c
    own = lax.rem(lax.axis_index("groups"), 2) if paired else 0
    other_group = lax.axis_index("groups") + 1 - 2 * own if paired else 0
    image_rows, width = image_tokens.shape
    text_rows = text_tokens.shape[0]
    local_rows = image_rows + text_rows
    slab = qkv_image.shape[0]
    columns = qkv_image.shape[1]
    size = columns // 3
    active = c == own

    def when_active(run):
        if paired:
            pl.when(active)(run)
        else:
            run()


    def wrap(i, n):
        return lax.rem(i + n, n)

    def copy_of(src, dst, sems, index, device):
        return pltpu.make_async_remote_copy(
            src_ref=src,
            dst_ref=dst,
            send_sem=sems[0].at[0],
            recv_sem=sems[1].at[index],
            device_id=device,
            device_id_type=MESH,
        )

    def send(src, dst, sems, index, device):
        copy_of(src, dst, sems, index, device).start()

    def arrive(ref, sems, index, device):
        copy_of(ref, ref, sems, index, device).wait_recv()

    def sent(ref, sems, index, device):
        copy_of(ref, ref, sems, index, device).wait_send()

    right, left = {"seq": wrap(z + 1, nz)}, {"seq": wrap(z - 1, nz)}
    partner = {"groups": other_group}
    sibling = {"sub": 1 - c}

    barrier = pltpu.get_barrier_semaphore()
    peers = [{"seq": wrap(z + i, nz)} for i in range(1, nz)]
    plane = [
        {"tensor": lax.div(wrap(me + i, heads), nc), "sub": lax.rem(wrap(me + i, heads), nc)}
        for i in range(1, heads)
    ]
    greeted = peers + plane + ([partner] if paired else [])
    for device in greeted:
        pl.semaphore_signal(barrier, inc=1, device_id=device, device_id_type=MESH)

    piece = 2 * slab
    table_window = pl.ds(pl.multiple_of(lax.div(z, 2) * piece, 128), piece)
    loads = [
        pltpu.make_async_copy(src, dst, load_sem.at[i])
        for i, (src, dst) in enumerate(
            (
                (table_hbm.at[:, table_window], time_table),
                (mod_hbm, mod_weight),
                (qkv_image, weights.at[z]),
                (qkv_text, text_weights.at[z]),
                (proj_image, proj_z.at[z, 0]),
                (proj_text, proj_z.at[z, 1]),
                (text_hbm, text_tokens),
                (image_hbm, image_tokens),
                (gain_hbm, norm_gain),
            )
        )
    ]
    for copy in loads:
        copy.start()
    for copy in loads[:6]:
        copy.wait()

    picked = lax.broadcasted_iota(jnp.int32, time_table.shape, 0) == timestep[0]
    embedded = jnp.sum(
        jnp.where(picked, time_table[...].astype(F32), 0.0), axis=0, keepdims=True
    )
    vector = (embedded / (1.0 + jnp.exp(-embedded))).astype(BF16)
    vector_rows = jnp.where(lax.rem(z, 2) == 0, vector[:, :slab], vector[:, slab:])
    mod_z[z] = jnp.dot(vector_rows, mod_weight[...], preferred_element_type=F32)

    chunk = 16

    def statistics(tokens, first, last, at):
        def one(i, carry):
            rows = rows_at(i * chunk, chunk)
            values = tokens[rows, :].astype(F32)
            center = jnp.mean(values, axis=-1, keepdims=True)
            spread = jnp.mean(jnp.square(values - center), axis=-1, keepdims=True)
            out = rows_at(at + i * chunk, chunk)
            mean_of[out, :] = jnp.broadcast_to(center, (chunk, 128))
            rstd_of[out, :] = jnp.broadcast_to(lax.rsqrt(spread + EPSILON), (chunk, 128))
            return carry

        lax.fori_loop(first // chunk, last // chunk, one, 0)

    pl.semaphore_wait(barrier, len(greeted))

    for i in range(1, nz):
        send(mod_z.at[z], mod_z.at[z], modz_sems, (0,), peers[i - 1])

    half = nz // 2

    def slab_of(way, d):
        return wrap(z - d, nz) if way == RIGHT else wrap(z + d, nz)

    def carried(way, d, part, parts):
        return d < half or (part < parts // 2) == (way == RIGHT)

    def ring_part(d, part, parts, part_ref, sems):
        for way, to in ((RIGHT, right), (LEFT, left)):
            if not carried(way, d, part, parts):
                continue
            here = part_ref(slab_of(way, d), part)
            if d > 0:
                arrive(here, sems, (way, d - 1, part), to)
            if d < half and carried(way, d + 1, part, parts):
                send(here, here, sems, (way, d, part), to)

    share = slab // 2 if paired else slab

    def w_part(block, part):
        return weights.at[block, rows_at(own * share + part * (share // 2), share // 2), :]

    def w_share(block, of):
        return weights.at[block, rows_at(of * share, share), :]

    def t_part(block, part):
        return text_weights.at[block, pl.ds(part * (slab // 2), slab // 2), :]

    def p_part(block, part):
        return proj_z.at[block, :, rows_at(own * share + part * (share // 2), share // 2), :]

    def p_share(ref, block):
        return ref.at[block, :, rows_at(own * share, share), :]

    def weight_step(d, tasks=((), ())):
        for part in (0, 1):
            ring_part(d, part, 2, w_part, w_sems)
            when_active(lambda: ring_part(d, part, 2, t_part, t_sems))
            if part == 0:
                for task in tasks[0]:
                    task()
        if paired and d > 0:
            for way in (RIGHT, LEFT):
                if way == RIGHT or d < half:
                    here = w_share(slab_of(way, d), own)
                    send(here, here, wy_sems, (way, d - 1), partner)
        for task in tasks[1]:
            task()

    def weight_wait(d):
        if paired:
            for way in (RIGHT, LEFT):
                if way == RIGHT or d < half:
                    arrive(w_share(slab_of(way, d), 1 - own), wy_sems, (way, d - 1), partner)

    weight_step(0)

    for copy in loads[6:]:
        copy.wait()
    statistics(text_tokens, 0, text_rows, image_rows)
    statistics(image_tokens, 0, image_rows // 2, 0)

    def mod_over_seq():
        arrive(mod_z.at[pl.ds(0, nz - 1)], modz_sems, (0,), right)
        total = mod_z[0]
        for i in range(1, nz):
            total = total + mod_z[i]
        mod_all[me] = total
        for device in plane:
            send(mod_all.at[me], mod_all.at[me], modx_sems, (0,), device)

    def mod_over_plane():
        arrive(mod_all.at[pl.ds(0, heads - 1)], modx_sems, (0,), sibling)

    per_block = mod_weight.shape[1] // piece
    pieces = width // piece

    def mod_piece(index):
        if isinstance(index, int):
            return mod_all[index // per_block, :, pl.ds(index % per_block * piece, piece)]
        offset = pl.multiple_of(lax.rem(index, per_block) * piece, 128)
        return mod_all[lax.div(index, per_block), :, pl.ds(offset, piece)]

    def hide(tokens, hidden, stream, first, last, at):
        def one(i, carry):
            rows = rows_at(i * chunk, chunk)
            out = rows_at(at + i * chunk, chunk)
            center, scale = mean_of[out, 0:1], rstd_of[out, 0:1]
            for p in range(pieces):
                shift = mod_piece((stream * 3) * pieces + p)
                scaling = mod_piece((stream * 3 + 1) * pieces + p)
                values = tokens[rows, p * piece : (p + 1) * piece].astype(F32)
                values = ((values - center) * scale * (1.0 + scaling) + shift).astype(BF16)
                hidden[2 * p, rows, :] = values[:, :slab]
                hidden[2 * p + 1, rows, :] = values[:, slab:]
            return carry

        lax.fori_loop(first // chunk, last // chunk, one, 0)

    sum_image[...] = jnp.zeros_like(sum_image)
    sum_text[...] = jnp.zeros_like(sum_text)

    def block_at(j):
        step = lax.div(j + 1, 2)
        return wrap(jnp.where(lax.rem(j, 2) == 1, z - step, z + step), nz)

    def project(hidden, total, shards, first, last):
        def one(j, carry):
            block = block_at(j)
            total[...] += jnp.dot(hidden[block], shards[block], preferred_element_type=F32)
            return carry

        lax.fori_loop(first, last, one, 0)

    def give_block(block):
        target = {"tensor": lax.div(block, nc), "sub": lax.rem(block, nc)}

        @pl.when(block != me)
        def _():
            send(p_share(proj_z, block), p_share(proj_all, me), px_sems, (0,), target)

        @pl.when(block == me)
        def _():
            rows = rows_at(own * share, share)
            proj_all[me, :, rows, :] = proj_z[block, :, rows, :]

    def proj_step(d):
        for part in (0, 1):
            ring_part(d, part, 2, p_part, p_sems)
        give_block(slab_of(RIGHT, d))
        if 0 < d < half:
            give_block(slab_of(LEFT, d))

    away = lax.rem(z - me + nz, nz)
    away = jnp.minimum(away, nz - away)
    all_shares = proj_all.at[:, :, rows_at(own * share, share), :]
    other_shares = proj_all.at[:, :, rows_at((1 - own) * share, share), :]

    def hand_over(d):
        @pl.when(away == d)
        def _():
            arrive(proj_all.at[pl.ds(0, heads - 1), :, pl.ds(0, share), :], px_sems, (0,), sibling)
            if paired:
                send(all_shares, all_shares, py_sems, (0,), partner)

    lag = min(5, half)
    proj_plan = {}
    for d in range(half + 1):
        proj_plan.setdefault(lag + d, []).append((proj_step, d))
        after = max(lag + d + 3, half + 1 + (d + 1) // 2)
        proj_plan.setdefault(min(after, 2 * half + 1), []).append((hand_over, d))

    def proj_advance(step):
        for call, d in proj_plan.get(step, ()):
            call(d)

    def hidden_exchange():
        if paired:

            @pl.when(jnp.logical_not(active))
            def _():
                send(both[0], both[1], th_sems, (0,), partner)

    both = (
        hidden_text.at[:, pl.ds(0, text_rows), :],
        hidden_text.at[:, pl.ds(text_rows, text_rows), :],
    )
    middle = image_rows // 2

    def project_all(first, last):
        project(hidden_image, sum_image, weights, first, last)
        when_active(lambda: project(hidden_text, sum_text, text_weights, first, last))

    def receive_hidden():
        if paired:
            when_active(lambda: arrive(both[1], th_sems, (0,), partner))

    def stats_of(first):
        return lambda: statistics(image_tokens, first, first + middle // 2, 0)

    def hide_of(first):
        return lambda: hide(image_tokens, hidden_image, 0, first, first + middle // 2, 0)

    def hide_text():
        mod_over_plane()
        hide(text_tokens, hidden_text, 1, 0, text_rows, image_rows)
        hidden_exchange()

    done = 0

    def multiply(until):
        def run():
            nonlocal done
            project_all(done, until)
            done = max(done, until)

        return run

    quarter_rows = middle // 2
    early = [
        (1, 0, stats_of(middle)),
        (1, 1, stats_of(middle + quarter_rows)),
        (2, 1, mod_over_seq),
        (4, 0, hide_text),
        (4, 1, hide_of(0)),
        (5, 0, hide_of(quarter_rows)),
        (5, 1, hide_of(middle)),
        (6, 0, hide_of(middle + quarter_rows)),
        (6, 0, receive_hidden),
    ]
    if half >= 8:
        early += [(6, 1, multiply(3)), (7, 0, multiply(6)), (7, 1, multiply(9)), (8, 0, multiply(11))]
    for d in range(1, half + 1):
        tasks = [
            [task for at, place, task in early if (min(at, half), place if at < half else 1) == (d, p)]
            if d < half or p == 1
            else []
            for p in (0, 1)
        ]
        weight_step(d, tasks)
        proj_advance(d)
        if d > 2:
            weight_wait(d - 2)
    for d in range(max(1, half - 1), half + 1):
        weight_wait(d)
        multiply(min(2 * d + 1, nz))()

    def normed(values, gain):
        return (
            values
            * lax.rsqrt(jnp.mean(values * values, axis=-1, keepdims=True) + EPSILON)
            * gain
        ).astype(BF16)

    def normed_three(total, stream):
        return (
            normed(total[:, 0:size], norm_gain[stream, 0]),
            normed(total[:, size : 2 * size], norm_gain[stream, 1]),
            total[:, 2 * size : 3 * size].astype(BF16),
        )

    quarter = local_rows // 64 * 16
    starts = (0, local_rows // 2 - quarter, local_rows // 2, local_rows - quarter, local_rows)

    def kv_part(block, part):
        return key_value.at[block, pl.ds(starts[part], starts[part + 1] - starts[part]), :]

    q, k, v = normed_three(sum_image[...], 0)
    query[0:image_rows, :] = q
    key_value[z, 0:image_rows, 0:size] = k
    key_value[z, 0:image_rows, size : 2 * size] = v
    for part in (0, 1, 2):
        ring_part(0, part, 4, kv_part, kv_sems)

    def text_projection():
        for side in (0, 1) if paired else (0,):
            parts = normed_three(sum_text[side * text_rows : (side + 1) * text_rows, :], 1)
            for i in range(3):
                text_qkv[side, :, i * size : (i + 1) * size] = parts[i]
        if paired:
            send(text_qkv.at[1], text_qkv.at[0], tq_sems, (0,), partner)

    when_active(text_projection)
    if paired:

        @pl.when(jnp.logical_not(active))
        def _():
            arrive(text_qkv.at[0], tq_sems, (0,), partner)

    query[image_rows:, :] = text_qkv[0, :, 0:size]
    key_value[z, image_rows:, :] = text_qkv[0, :, size : 3 * size]
    ring_part(0, 3, 4, kv_part, kv_sems)

    row_max[...] = jnp.full_like(row_max, -1e30)
    row_sum[...] = jnp.zeros_like(row_sum)
    mixed[...] = jnp.zeros_like(mixed)
    factor = float(size) ** (-0.5) * math.log2(math.e)

    def attend(first, last):
        def one(j, carry):
            block = block_at(j)
            scores = lax.dot_general(
                query[...],
                key_value[block, :, 0:size],
                (((1,), (1,)), ((), ())),
                preferred_element_type=F32,
            )
            within = lax.broadcasted_iota(jnp.int32, scores.shape, 1)
            slot = block * text_rows + within - image_rows
            usable = (within < image_rows) | (slot < text_length[0])
            scores = jnp.where(usable, scores, -1e30)
            old = row_max[:, 0:1]
            new = jnp.maximum(old, jnp.max(scores, axis=-1, keepdims=True))
            probs = jnp.exp2((scores - new) * factor)
            fade = jnp.exp2((old - new) * factor)
            row_max[...] = jnp.broadcast_to(new, row_max.shape)
            total = row_sum[:, 0:1] * fade + jnp.sum(probs, axis=-1, keepdims=True)
            row_sum[...] = jnp.broadcast_to(total, row_sum.shape)
            mixed[...] = mixed[...] * fade + jnp.dot(
                probs.astype(BF16),
                key_value[block, :, size : 2 * size],
                preferred_element_type=F32,
            )
            return carry

        lax.fori_loop(first, last, one, 0)

    for d in range(1, half + 1):
        for part in (0, 1):
            ring_part(d, part, 4, kv_part, kv_sems)
        attend(max(2 * d - 3, 0), 2 * d - 2 if d > 1 else 1)
        for part in (2, 3):
            ring_part(d, part, 4, kv_part, kv_sems)
        proj_advance(half + d)
        if d > 1:
            attend(2 * d - 2, 2 * d - 1)
    proj_advance(2 * half + 1)
    attend(nz - 1, nz)

    attended[me] = (mixed[...] / row_sum[:, 0:1]).astype(BF16)

    x_half = nx // 2
    x_right, x_left = {"tensor": wrap(x + 1, nx)}, {"tensor": wrap(x - 1, nx)}
    half_rows = local_rows // 2

    def x_carried(way, d, part):
        return d < x_half or (part == 0) == (way == RIGHT)

    def x_block(way, d):
        return (wrap(x - d, nx) if way == RIGHT else wrap(x + d, nx)) * nc + c

    def a_part(block, part):
        return attended.at[block, pl.ds(part * half_rows, half_rows), :]

    for d in range(0, x_half + 1):
        for part in (0, 1):
            for way, to in ((RIGHT, x_right), (LEFT, x_left)):
                if not x_carried(way, d, part):
                    continue
                here = a_part(x_block(way, d), part)
                if d > 0:
                    arrive(here, ax_sems, (way, d - 1, part), to)
                if d < x_half and x_carried(way, d + 1, part):
                    send(here, here, ax_sems, (way, d, part), to)
                if d > 0 or way == RIGHT:
                    send(here, here, as_sems, (way, d, part), sibling)

    if paired:
        arrive(other_shares, py_sems, (0,), partner)

    across = 1 - 2 * c
    for d in range(0, x_half + 1):
        for part in (0, 1):
            for way in (RIGHT, LEFT):
                if x_carried(way, d, part) and (d > 0 or way == RIGHT):
                    arrive(
                        a_part(x_block(way, d) + across, part), as_sems, (way, d, part), sibling
                    )

    out_width = image_out.shape[1]
    image_sum, text_sum = None, None
    for h in range(0, heads, 2):
        rows = jnp.concatenate([attended[h], attended[h + 1]], axis=1)
        image_w = jnp.concatenate([proj_all[h, 0], proj_all[h + 1, 0]], axis=1)
        text_w = jnp.concatenate([proj_all[h, 1], proj_all[h + 1, 1]], axis=1)
        turned = (((1,), (1,)), ((), ()))
        image_term = lax.dot_general(
            rows[:image_rows], image_w, turned, preferred_element_type=F32
        )
        text_term = lax.dot_general(rows[image_rows:], text_w, turned, preferred_element_type=F32)
        image_sum = image_term if image_sum is None else image_sum + image_term
        text_sum = text_term if text_sum is None else text_sum + text_term

    def own_columns(wide):
        return jnp.where(c == 0, wide[:, :out_width], wide[:, out_width:])

    window = pl.ds(pl.multiple_of(x * 2 * out_width, 128), 2 * out_width)
    for tokens, total, out, stream in (
        (image_tokens, image_sum, image_out, 0),
        (text_tokens, text_sum, text_out, 1),
    ):
        gate = own_columns(mod_piece((stream * 3 + 2) * pieces + x))
        base = own_columns(tokens[:, window].astype(F32))
        out[...] = (base + gate * total).astype(BF16)

    sent(mod_z.at[pl.ds(0, nz - 1)], modz_sems, (0,), right)
    sent(mod_all.at[pl.ds(0, heads - 1)], modx_sems, (0,), sibling)
    blocks = pl.ds(0, nz - 1)
    sent(weights.at[blocks, pl.ds(0, share), :], w_sems, (0, 0, 0), right)
    sent(proj_z.at[blocks, :, pl.ds(0, share), :], p_sems, (0, 0, 0), right)
    sent(proj_all.at[pl.ds(0, heads - 1), :, pl.ds(0, share), :], px_sems, (0,), sibling)
    sent(key_value.at[blocks], kv_sems, (0, 0, 0), right)
    sent(attended.at[pl.ds(0, nx - 1)], ax_sems, (0, 0, 0), x_right)
    sent(attended.at[pl.ds(0, nx)], as_sems, (0, 0, 0), sibling)
    if paired:
        sent(weights.at[blocks, pl.ds(0, share), :], wy_sems, (0, 0), partner)
        sent(all_shares, py_sems, (0,), partner)

    def text_sent():
        sent(text_weights.at[blocks], t_sems, (0, 0, 0), right)
        if paired:
            sent(text_qkv.at[1], tq_sems, (0,), partner)

    when_active(text_sent)
    if paired:

        @pl.when(jnp.logical_not(active))
        def _():
            sent(both[0], th_sems, (0,), partner)


def solution(mesh):
    nz, nx, nc = mesh.shape["seq"], mesh.shape["tensor"], mesh.shape["sub"]
    paired = mesh.shape["groups"] % 2 == 0
    heads = nx * nc

    def body(
        image_tokens,
        text_tokens,
        timestep,
        text_length,
        time_table,
        mod_weight,
        qkv_image,
        qkv_text,
        norm_gain,
        proj_image,
        proj_text,
    ):
        slab = qkv_image.shape[0]
        gains = norm_gain.reshape(2, 2, 1, norm_gain.shape[-1])
        image_rows, width = image_tokens.shape
        text_rows = text_tokens.shape[0]
        local_rows = image_rows + text_rows
        columns = qkv_image.shape[1]
        size = columns // 3
        out_width = width // heads
        half = nz // 2
        vmem = pl.BlockSpec(memory_space=pltpu.VMEM)
        anywhere = pl.BlockSpec(memory_space=pl.ANY)
        dma = pltpu.SemaphoreType.DMA

        def pair(*shape):
            return dma((1,)), dma(shape)

        return pl.pallas_call(
            functools.partial(kernel, (nz, nx, nc), paired),
            out_shape=(
                jax.ShapeDtypeStruct((image_rows, out_width), BF16),
                jax.ShapeDtypeStruct((text_rows, out_width), BF16),
            ),
            in_specs=[pl.BlockSpec(memory_space=pltpu.SMEM)] * 2 + [anywhere] * 9,
            out_specs=(vmem, vmem),
            scratch_shapes=[
                pltpu.VMEM(image_tokens.shape, BF16),
                pltpu.VMEM(text_tokens.shape, BF16),
                pltpu.VMEM((time_table.shape[0], 2 * slab), BF16),
                pltpu.VMEM(mod_weight.shape, BF16),
                pltpu.VMEM(gains.shape, F32),
                pltpu.VMEM((nz, 1, mod_weight.shape[1]), F32),
                pltpu.VMEM((heads, 1, mod_weight.shape[1]), F32),
                pltpu.VMEM((local_rows, 128), F32),
                pltpu.VMEM((local_rows, 128), F32),
                pltpu.VMEM((nz, image_rows, slab), BF16),
                pltpu.VMEM((nz, 2 * text_rows, slab), BF16),
                pltpu.VMEM((nz, slab, columns), BF16),
                pltpu.VMEM((nz, slab, columns), BF16),
                pltpu.VMEM((image_rows, columns), F32),
                pltpu.VMEM((2 * text_rows, columns), F32),
                pltpu.VMEM((2, text_rows, columns), BF16),
                pltpu.VMEM((nz, 2, *proj_image.shape[::-1]), BF16),
                pltpu.VMEM((heads, 2, *proj_image.shape[::-1]), BF16),
                pltpu.VMEM((local_rows, size), BF16),
                pltpu.VMEM((nz, local_rows, 2 * size), BF16),
                pltpu.VMEM((local_rows, 128), F32),
                pltpu.VMEM((local_rows, 128), F32),
                pltpu.VMEM((local_rows, size), F32),
                pltpu.VMEM((heads, local_rows, size), BF16),
                dma((9,)),
                *pair(1),
                *pair(1),
                *pair(2, half, 2),
                *pair(2, half),
                *pair(2, half, 2),
                *pair(1),
                *pair(1),
                *pair(2, half, 2),
                *pair(1),
                *pair(1),
                *pair(2, half, 4),
                *pair(2, nx // 2, 2),
                *pair(2, nx // 2 + 1, 2),
            ],
            compiler_params=pltpu.CompilerParams(
                collective_id=0, has_side_effects=True, vmem_limit_bytes=56 * 1024 * 1024
            ),
        )(
            text_length,
            timestep,
            image_tokens,
            text_tokens,
            time_table,
            mod_weight,
            gains,
            qkv_image,
            qkv_text,
            proj_image.T,
            proj_text.T,
        )

    return jax.shard_map(
        body,
        mesh=mesh,
        in_specs=(
            P(("groups", "seq"), None),
            P(("groups", "seq"), None),
            P("groups"),
            P("groups"),
            P(),
            P("seq", ("tensor", "sub")),
            P("seq", ("tensor", "sub")),
            P("seq", ("tensor", "sub")),
            P(None, None, ("tensor", "sub"), None),
            P(("tensor", "sub"), "seq"),
            P(("tensor", "sub"), "seq"),
        ),
        out_specs=(
            P(("groups", "seq"), ("tensor", "sub")),
            P(("groups", "seq"), ("tensor", "sub")),
        ),
        check_vma=False,
    )
```

```python
import functools
import math

import jax
import jax.numpy as jnp
from jax import lax
from jax.experimental import pallas as pl
from jax.experimental.pallas import tpu as pltpu
from jax.sharding import PartitionSpec as P

EPSILON = 1e-06
MESH = pl.DeviceIdType.MESH
BF16 = jnp.bfloat16
F32 = jnp.float32
RIGHT, LEFT = 0, 1


def rows_at(start, size, unit=16):
    if isinstance(start, int):
        return pl.ds(start, size)
    return pl.ds(pl.multiple_of(start, unit), size)


def kernel(
    sizes,
    paired,
    length_hbm,
    step_hbm,
    image_hbm,
    text_hbm,
    table_hbm,
    mod_hbm,
    gain_hbm,
    qkv_image,
    qkv_text,
    proj_image,
    proj_text,
    image_out,
    text_out,
    image_tokens,
    text_tokens,
    time_table,
    mod_weight,
    norm_gain,
    mod_rows,
    mod_in,
    mod_all,
    mean_of,
    rstd_of,
    hidden_image,
    hidden_text,
    weights,
    text_weights,
    sum_image,
    sum_text,
    text_qkv,
    proj_z,
    proj_all,
    query,
    key_value,
    row_max,
    row_sum,
    mixed,
    attended,
    text_length,
    timestep,
    load_sem,
    mod_sems,
    *pairs,
):
    nz, nx, nc = sizes
    (
        modx_sems,
        w_sems,
        wy_sems,
        t_sems,
        th_sems,
        tq_sems,
        p_sems,
        py_sems,
        px_sems,
        kv_sems,
        ax_sems,
        as_sems,
    ) = zip(pairs[0::2], pairs[1::2])
    heads = nx * nc
    z = lax.axis_index("seq")
    x = lax.axis_index("tensor")
    c = lax.axis_index("sub")
    me = x * nc + c
    own = lax.rem(lax.axis_index("groups"), 2) if paired else 0
    other_group = lax.axis_index("groups") + 1 - 2 * own if paired else 0
    image_rows, width = image_tokens.shape
    text_rows = text_tokens.shape[0]
    local_rows = image_rows + text_rows
    slab = qkv_image.shape[0]
    columns = qkv_image.shape[1]
    size = columns // 3
    active = c == own

    def when_active(run):
        if paired:
            pl.when(active)(run)
        else:
            run()


    def wrap(i, n):
        return lax.rem(i + n, n)

    def copy_of(src, dst, sems, index, device):
        return pltpu.make_async_remote_copy(
            src_ref=src,
            dst_ref=dst,
            send_sem=sems[0].at[0],
            recv_sem=sems[1].at[index],
            device_id=device,
            device_id_type=MESH,
        )

    def send(src, dst, sems, index, device):
        copy_of(src, dst, sems, index, device).start()

    def arrive(ref, sems, index, device):
        copy_of(ref, ref, sems, index, device).wait_recv()

    def sent(ref, sems, index, device):
        copy_of(ref, ref, sems, index, device).wait_send()

    right, left = {"seq": wrap(z + 1, nz)}, {"seq": wrap(z - 1, nz)}
    partner = {"groups": other_group}
    sibling = {"sub": 1 - c}

    barrier = pltpu.get_barrier_semaphore()
    peers = [{"seq": wrap(z + i, nz)} for i in range(1, nz)]
    plane = [
        {"tensor": lax.div(wrap(me + i, heads), nc), "sub": lax.rem(wrap(me + i, heads), nc)}
        for i in range(1, heads)
    ]
    greeted = peers + plane + ([partner] if paired else [])
    for device in greeted:
        pl.semaphore_signal(barrier, inc=1, device_id=device, device_id_type=MESH)

    piece = 2 * slab
    table_window = pl.ds(pl.multiple_of(lax.div(z, 2) * piece, 128), piece)
    loads = [
        pltpu.make_async_copy(src, dst, load_sem.at[i])
        for i, (src, dst) in enumerate(
            (
                (step_hbm, timestep),
                (length_hbm, text_length),
                (table_hbm.at[:, table_window], time_table),
                (mod_hbm, mod_weight),
                (qkv_image, weights.at[rows_at(z * slab, slab), :]),
                (qkv_text, text_weights.at[rows_at(z * slab, slab), :]),
                (proj_image, proj_z.at[z, 0]),
                (proj_text, proj_z.at[z, 1]),
                (text_hbm, text_tokens),
                (image_hbm, image_tokens),
                (gain_hbm, norm_gain),
            )
        )
    ]
    for copy in loads:
        copy.start()
    for copy in loads[:8]:
        copy.wait()

    picked = lax.broadcasted_iota(jnp.int32, time_table.shape, 0) == timestep[0]
    embedded = jnp.sum(
        jnp.where(picked, time_table[...].astype(F32), 0.0), axis=0, keepdims=True
    )
    vector = (embedded / (1.0 + jnp.exp(-embedded))).astype(BF16)
    vector_rows = jnp.where(lax.rem(z, 2) == 0, vector[:, :slab], vector[:, slab:])
    partial_sum = jnp.dot(vector_rows, mod_weight[...], preferred_element_type=F32)
    chunks = partial_sum.shape[1] // 128
    for i in range(chunks):
        mod_rows[i] = partial_sum[:, i * 128 : (i + 1) * 128]

    chunk = 16

    def statistics(tokens, first, last, at):
        def one(i, carry):
            rows = rows_at(i * chunk, chunk)
            values = tokens[rows, :].astype(F32)
            center = jnp.mean(values, axis=-1, keepdims=True)
            spread = jnp.mean(jnp.square(values - center), axis=-1, keepdims=True)
            out = rows_at(at + i * chunk, chunk)
            mean_of[out, :] = jnp.broadcast_to(center, (chunk, 128))
            rstd_of[out, :] = jnp.broadcast_to(lax.rsqrt(spread + EPSILON), (chunk, 128))
            return carry

        lax.fori_loop(first // chunk, last // chunk, one, 0)

    pl.semaphore_wait(barrier, len(greeted))

    def is_owner(i):
        return z == i % nz

    def mod_copy(i, src, dst, stage, device):
        return pltpu.make_async_remote_copy(
            src_ref=src,
            dst_ref=dst,
            send_sem=mod_sems.at[0, stage, i],
            recv_sem=mod_sems.at[1, stage, i],
            device_id=device,
            device_id_type=MESH,
        )

    def mod_total(i):
        return mod_all.at[me, :, pl.ds(i * 128, 128)]

    def mod_partial():
        for i in range(chunks):

            @pl.when(jnp.logical_not(is_owner(i)))
            def _():
                mod_copy(i, mod_rows.at[i], mod_in.at[i, z], 0, {"seq": i % nz}).start()

            @pl.when(is_owner(i))
            def _():
                mod_in[i, z] = mod_rows[i]

    def mod_reduce():
        for i in range(chunks):
            others = mod_in.at[i, pl.ds(0, nz - 1)]

            @pl.when(is_owner(i))
            def _():
                mod_copy(i, others, others, 0, right).wait_recv()
                total = mod_in[i, 0]
                for k in range(1, nz):
                    total = total + mod_in[i, k]
                mod_all[me, :, i * 128 : (i + 1) * 128] = total
                for device in peers:
                    mod_copy(i, mod_total(i), mod_total(i), 1, device).start()

    def mod_sent():
        for i in range(chunks):
            others = mod_in.at[i, pl.ds(0, nz - 1)]

            @pl.when(jnp.logical_not(is_owner(i)))
            def _():
                mod_copy(i, mod_rows.at[i], mod_rows.at[i], 0, right).wait_send()

            @pl.when(is_owner(i))
            def _():
                mod_copy(i, others, others, 1, right).wait_send()

    mod_partial()

    half = nz // 2

    def slab_of(way, d):
        return wrap(z - d, nz) if way == RIGHT else wrap(z + d, nz)

    def carried(way, d, part, parts):
        return d < half or (part < parts // 2) == (way == RIGHT)

    def ring_part(d, part, parts, part_ref, sems):
        for way, to in ((RIGHT, right), (LEFT, left)):
            if not carried(way, d, part, parts):
                continue
            here = part_ref(slab_of(way, d), part)
            if d > 0:
                arrive(here, sems, (way, d - 1, part), to)
            if d < half and carried(way, d + 1, part, parts):
                send(here, here, sems, (way, d, part), to)

    share = slab // 2 if paired else slab

    def w_part(block, part):
        start = block * slab + own * share + part * (share // 2)
        return weights.at[rows_at(start, share // 2), :]

    def w_share(block, of):
        return weights.at[rows_at(block * slab + of * share, share), :]

    def t_part(block, part):
        return text_weights.at[rows_at(block * slab + part * (slab // 2), slab // 2), :]

    def p_part(block, part):
        return proj_z.at[block, :, rows_at(own * share + part * (share // 2), share // 2), :]

    def p_share(ref, block):
        return ref.at[block, :, rows_at(own * share, share), :]

    def weight_step(d, tasks=((), ())):
        for part in (0, 1):
            ring_part(d, part, 2, w_part, w_sems)
            when_active(lambda: ring_part(d, part, 2, t_part, t_sems))
            if part == 0:
                for task in tasks[0]:
                    task()
        if paired and d > 0:
            for way in (RIGHT, LEFT):
                if way == RIGHT or d < half:
                    here = w_share(slab_of(way, d), own)
                    send(here, here, wy_sems, (way, d - 1), partner)
        for task in tasks[1]:
            task()

    def weight_wait(d):
        if paired:
            for way in (RIGHT, LEFT):
                if way == RIGHT or d < half:
                    arrive(w_share(slab_of(way, d), 1 - own), wy_sems, (way, d - 1), partner)

    weight_step(0)

    for copy in loads[8:]:
        copy.wait()
    statistics(text_tokens, 0, text_rows, image_rows)
    statistics(image_tokens, 0, image_rows // 2, 0)

    def mod_over_seq():
        for i in range(chunks):

            @pl.when(jnp.logical_not(is_owner(i)))
            def _():
                mod_copy(i, mod_total(i), mod_total(i), 1, right).wait_recv()

        for device in plane:
            send(mod_all.at[me], mod_all.at[me], modx_sems, (0,), device)

    def mod_over_plane():
        arrive(mod_all.at[pl.ds(0, heads - 1)], modx_sems, (0,), sibling)

    per_block = mod_weight.shape[1] // piece
    pieces = width // piece

    def mod_piece(index):
        if isinstance(index, int):
            return mod_all[index // per_block, :, pl.ds(index % per_block * piece, piece)]
        offset = pl.multiple_of(lax.rem(index, per_block) * piece, 128)
        return mod_all[lax.div(index, per_block), :, pl.ds(offset, piece)]

    def hide(tokens, hidden, stream, first, last, at):
        def one(i, carry):
            rows = rows_at(i * chunk, chunk)
            out = rows_at(at + i * chunk, chunk)
            center, scale = mean_of[out, 0:1], rstd_of[out, 0:1]
            for p in range(pieces):
                shift = mod_piece((stream * 3) * pieces + p)
                scaling = mod_piece((stream * 3 + 1) * pieces + p)
                values = tokens[rows, p * piece : (p + 1) * piece].astype(F32)
                values = ((values - center) * scale * (1.0 + scaling) + shift).astype(BF16)
                hidden[rows, p * piece : (p + 1) * piece] = values
            return carry

        lax.fori_loop(first // chunk, last // chunk, one, 0)

    depth = 4 * slab

    def block_at(j):
        step = lax.div(j + 1, 2)
        return wrap(jnp.where(lax.rem(j, 2) == 1, z - step, z + step), nz)

    def project(hidden, total, shards):
        total[...] = jnp.zeros_like(total)

        def one(i, carry):
            at = pl.ds(pl.multiple_of(i * depth, 128), depth)
            total[...] += jnp.dot(hidden[:, at], shards[at, :], preferred_element_type=F32)
            return carry

        lax.fori_loop(0, nz * slab // depth, one, 0)

    def give_block(block):
        target = {"tensor": lax.div(block, nc), "sub": lax.rem(block, nc)}

        @pl.when(block != me)
        def _():
            send(p_share(proj_z, block), p_share(proj_all, me), px_sems, (0,), target)

        @pl.when(block == me)
        def _():
            rows = rows_at(own * share, share)
            proj_all[me, :, rows, :] = proj_z[block, :, rows, :]

    def proj_step(d):
        for part in (0, 1):
            ring_part(d, part, 2, p_part, p_sems)
        give_block(slab_of(RIGHT, d))
        if 0 < d < half:
            give_block(slab_of(LEFT, d))

    away = lax.rem(z - me + nz, nz)
    away = jnp.minimum(away, nz - away)
    all_shares = proj_all.at[:, :, rows_at(own * share, share), :]
    other_shares = proj_all.at[:, :, rows_at((1 - own) * share, share), :]

    def hand_over(d):
        @pl.when(away == d)
        def _():
            arrive(proj_all.at[pl.ds(0, heads - 1), :, pl.ds(0, share), :], px_sems, (0,), sibling)
            if paired:
                send(all_shares, all_shares, py_sems, (0,), partner)

    lag = min(5, half)
    proj_plan = {}
    for d in range(half + 1):
        proj_plan.setdefault(lag + d, []).append((proj_step, d))
        after = max(lag + d + 3, half + 1 + (d + 1) // 2)
        proj_plan.setdefault(min(after, 2 * half + 1), []).append((hand_over, d))

    def proj_advance(step):
        for call, d in proj_plan.get(step, ()):
            call(d)

    def hidden_exchange():
        if paired:

            @pl.when(jnp.logical_not(active))
            def _():
                send(both[0], both[1], th_sems, (0,), partner)

    both = (
        hidden_text.at[pl.ds(0, text_rows), :],
        hidden_text.at[pl.ds(text_rows, text_rows), :],
    )
    middle = image_rows // 2

    def stats_of(first):
        return lambda: statistics(image_tokens, first, first + middle // 2, 0)

    def hide_of(first):
        return lambda: hide(image_tokens, hidden_image, 0, first, first + middle // 2, 0)

    def hide_text():
        mod_over_plane()
        hide(text_tokens, hidden_text, 1, 0, text_rows, image_rows)
        hidden_exchange()

    quarter_rows = middle // 2
    early = [
        (1, 0, stats_of(middle)),
        (1, 1, stats_of(middle + quarter_rows)),
        (2, 1, mod_reduce),
        (4, 1, mod_over_seq),
        (6, 0, hide_text),
        (6, 1, hide_of(0)),
        (7, 0, hide_of(quarter_rows)),
        (7, 1, hide_of(middle)),
        (8, 1, hide_of(middle + quarter_rows)),
    ]
    for d in range(1, half + 1):
        tasks = [
            [task for at, place, task in early if (min(at, half), place if at < half else 1) == (d, p)]
            if d < half or p == 1
            else []
            for p in (0, 1)
        ]
        weight_step(d, tasks)
        proj_advance(d)
        if d > 2:
            weight_wait(d - 2)
    for d in range(max(1, half - 1), half + 1):
        weight_wait(d)
    project(hidden_image, sum_image, weights)

    def normed(values, gain):
        return (
            values
            * lax.rsqrt(jnp.mean(values * values, axis=-1, keepdims=True) + EPSILON)
            * gain
        ).astype(BF16)

    def normed_three(total, stream):
        return (
            normed(total[:, 0:size], norm_gain[stream, 0]),
            normed(total[:, size : 2 * size], norm_gain[stream, 1]),
            total[:, 2 * size : 3 * size].astype(BF16),
        )

    quarter = local_rows // 64 * 16
    starts = (0, local_rows // 2 - quarter, local_rows // 2, local_rows - quarter, local_rows)

    def kv_part(block, part):
        return key_value.at[block, pl.ds(starts[part], starts[part + 1] - starts[part]), :]

    q, k, v = normed_three(sum_image[...], 0)
    query[0:image_rows, :] = q
    key_value[z, 0:image_rows, 0:size] = k
    key_value[z, 0:image_rows, size : 2 * size] = v
    for part in (0, 1, 2):
        ring_part(0, part, 4, kv_part, kv_sems)

    def text_projection():
        if paired:
            arrive(both[1], th_sems, (0,), partner)
        project(hidden_text, sum_text, text_weights)
        for side in (0, 1) if paired else (0,):
            parts = normed_three(sum_text[side * text_rows : (side + 1) * text_rows, :], 1)
            for i in range(3):
                text_qkv[side, :, i * size : (i + 1) * size] = parts[i]
        if paired:
            send(text_qkv.at[1], text_qkv.at[0], tq_sems, (0,), partner)

    when_active(text_projection)
    if paired:

        @pl.when(jnp.logical_not(active))
        def _():
            arrive(text_qkv.at[0], tq_sems, (0,), partner)

    query[image_rows:, :] = text_qkv[0, :, 0:size]
    key_value[z, image_rows:, :] = text_qkv[0, :, size : 3 * size]
    ring_part(0, 3, 4, kv_part, kv_sems)

    row_max[...] = jnp.full_like(row_max, -1e30)
    row_sum[...] = jnp.zeros_like(row_sum)
    mixed[...] = jnp.zeros_like(mixed)
    factor = float(size) ** (-0.5) * math.log2(math.e)

    def attend(first, last):
        def one(j, carry):
            block = block_at(j)
            scores = lax.dot_general(
                query[...],
                key_value[block, :, 0:size],
                (((1,), (1,)), ((), ())),
                preferred_element_type=F32,
            )
            within = lax.broadcasted_iota(jnp.int32, scores.shape, 1)
            slot = block * text_rows + within - image_rows
            usable = (within < image_rows) | (slot < text_length[0])
            scores = jnp.where(usable, scores, -1e30)
            old = row_max[:, 0:1]
            new = jnp.maximum(old, jnp.max(scores, axis=-1, keepdims=True))
            probs = jnp.exp2((scores - new) * factor)
            fade = jnp.exp2((old - new) * factor)
            row_max[...] = jnp.broadcast_to(new, row_max.shape)
            total = row_sum[:, 0:1] * fade + jnp.sum(probs, axis=-1, keepdims=True)
            row_sum[...] = jnp.broadcast_to(total, row_sum.shape)
            mixed[...] = mixed[...] * fade + jnp.dot(
                probs.astype(BF16),
                key_value[block, :, size : 2 * size],
                preferred_element_type=F32,
            )
            return carry

        lax.fori_loop(first, last, one, 0)

    for d in range(1, half + 1):
        for part in (0, 1):
            ring_part(d, part, 4, kv_part, kv_sems)
        attend(max(2 * d - 3, 0), 2 * d - 2 if d > 1 else 1)
        for part in (2, 3):
            ring_part(d, part, 4, kv_part, kv_sems)
        proj_advance(half + d)
        if d > 1:
            attend(2 * d - 2, 2 * d - 1)
    proj_advance(2 * half + 1)
    attend(nz - 1, nz)

    attended[me] = (mixed[...] / row_sum[:, 0:1]).astype(BF16)

    x_half = nx // 2
    x_right, x_left = {"tensor": wrap(x + 1, nx)}, {"tensor": wrap(x - 1, nx)}
    half_rows = local_rows // 2

    def x_carried(way, d, part):
        return d < x_half or (part == 0) == (way == RIGHT)

    def x_block(way, d):
        return (wrap(x - d, nx) if way == RIGHT else wrap(x + d, nx)) * nc + c

    def a_part(block, part):
        return attended.at[block, pl.ds(part * half_rows, half_rows), :]

    for d in range(0, x_half + 1):
        for part in (0, 1):
            for way, to in ((RIGHT, x_right), (LEFT, x_left)):
                if not x_carried(way, d, part):
                    continue
                here = a_part(x_block(way, d), part)
                if d > 0:
                    arrive(here, ax_sems, (way, d - 1, part), to)
                if d < x_half and x_carried(way, d + 1, part):
                    send(here, here, ax_sems, (way, d, part), to)
                if d > 0 or way == RIGHT:
                    send(here, here, as_sems, (way, d, part), sibling)

    if paired:
        arrive(other_shares, py_sems, (0,), partner)

    across = 1 - 2 * c
    for d in range(0, x_half + 1):
        for part in (0, 1):
            for way in (RIGHT, LEFT):
                if x_carried(way, d, part) and (d > 0 or way == RIGHT):
                    arrive(
                        a_part(x_block(way, d) + across, part), as_sems, (way, d, part), sibling
                    )

    out_width = text_out.shape[1]
    image_sum, text_sum = None, None
    for h in range(0, heads, 2):
        rows = jnp.concatenate([attended[h], attended[h + 1]], axis=1)
        image_w = jnp.concatenate([proj_all[h, 0], proj_all[h + 1, 0]], axis=1)
        text_w = jnp.concatenate([proj_all[h, 1], proj_all[h + 1, 1]], axis=1)
        turned = (((1,), (1,)), ((), ()))
        image_term = lax.dot_general(
            rows[:image_rows], image_w, turned, preferred_element_type=F32
        )
        text_term = lax.dot_general(rows[image_rows:], text_w, turned, preferred_element_type=F32)
        image_sum = image_term if image_sum is None else image_sum + image_term
        text_sum = text_term if text_sum is None else text_sum + text_term

    def own_columns(wide):
        return jnp.where(c == 0, wide[:, :out_width], wide[:, out_width:])

    window = pl.ds(pl.multiple_of(x * 2 * out_width, 128), 2 * out_width)
    for tokens, total, out, stream in (
        (image_tokens, image_sum, image_out, 0),
        (text_tokens, text_sum, text_out, 1),
    ):
        gate = own_columns(mod_piece((stream * 3 + 2) * pieces + x))
        base = own_columns(tokens[:, window].astype(F32))
        result = base + gate * total
        out[...] = (jnp.transpose(result) if stream == 0 else result).astype(BF16)

    mod_sent()
    sent(mod_all.at[pl.ds(0, heads - 1)], modx_sems, (0,), sibling)
    blocks = pl.ds(0, nz - 1)
    sent(weights.at[pl.ds(0, (nz - 1) * share), :], w_sems, (0, 0, 0), right)
    sent(proj_z.at[blocks, :, pl.ds(0, share), :], p_sems, (0, 0, 0), right)
    sent(proj_all.at[pl.ds(0, heads - 1), :, pl.ds(0, share), :], px_sems, (0,), sibling)
    sent(key_value.at[blocks], kv_sems, (0, 0, 0), right)
    sent(attended.at[pl.ds(0, nx - 1)], ax_sems, (0, 0, 0), x_right)
    sent(attended.at[pl.ds(0, nx)], as_sems, (0, 0, 0), sibling)
    if paired:
        sent(weights.at[pl.ds(0, (nz - 1) * share), :], wy_sems, (0, 0), partner)
        sent(all_shares, py_sems, (0,), partner)

    def text_sent():
        sent(text_weights.at[pl.ds(0, (nz - 1) * slab), :], t_sems, (0, 0, 0), right)
        if paired:
            sent(text_qkv.at[1], tq_sems, (0,), partner)

    when_active(text_sent)
    if paired:

        @pl.when(jnp.logical_not(active))
        def _():
            sent(both[0], th_sems, (0,), partner)


def hand_out(image, text, image_out, text_out):
    image_out[...] = image[...]
    text_out[...] = text[...]


def solution(mesh):
    nz, nx, nc = mesh.shape["seq"], mesh.shape["tensor"], mesh.shape["sub"]
    paired = mesh.shape["groups"] % 2 == 0
    heads = nx * nc

    def body(
        image_tokens,
        text_tokens,
        timestep,
        text_length,
        time_table,
        mod_weight,
        qkv_image,
        qkv_text,
        norm_gain,
        proj_image,
        proj_text,
    ):
        slab = qkv_image.shape[0]
        gains = norm_gain.reshape(2, 2, 1, norm_gain.shape[-1])
        image_rows, width = image_tokens.shape
        text_rows = text_tokens.shape[0]
        local_rows = image_rows + text_rows
        columns = qkv_image.shape[1]
        size = columns // 3
        out_width = width // heads
        half = nz // 2
        vmem = pl.BlockSpec(memory_space=pltpu.VMEM)
        anywhere = pl.BlockSpec(memory_space=pl.ANY)
        dma = pltpu.SemaphoreType.DMA

        def pair(*shape):
            return dma((1,)), dma(shape)

        results = pl.pallas_call(
            functools.partial(kernel, (nz, nx, nc), paired),
            out_shape=(
                jax.ShapeDtypeStruct((out_width, image_rows), BF16),
                jax.ShapeDtypeStruct((text_rows, out_width), BF16),
            ),
            in_specs=[pl.BlockSpec(memory_space=pltpu.HBM)] * 2 + [anywhere] * 9,
            out_specs=(vmem, vmem),
            scratch_shapes=[
                pltpu.VMEM(image_tokens.shape, BF16),
                pltpu.VMEM(text_tokens.shape, BF16),
                pltpu.VMEM((time_table.shape[0], 2 * slab), BF16),
                pltpu.VMEM(mod_weight.shape, BF16),
                pltpu.VMEM(gains.shape, F32),
                pltpu.VMEM((mod_weight.shape[1] // 128, 1, 128), F32),
                pltpu.VMEM((mod_weight.shape[1] // 128, nz, 1, 128), F32),
                pltpu.VMEM((heads, 1, mod_weight.shape[1]), F32),
                pltpu.VMEM((local_rows, 128), F32),
                pltpu.VMEM((local_rows, 128), F32),
                pltpu.VMEM((image_rows, width), BF16),
                pltpu.VMEM((2 * text_rows, width), BF16),
                pltpu.VMEM((width, columns), BF16),
                pltpu.VMEM((width, columns), BF16),
                pltpu.VMEM((image_rows, columns), F32),
                pltpu.VMEM((2 * text_rows, columns), F32),
                pltpu.VMEM((2, text_rows, columns), BF16),
                pltpu.VMEM((nz, 2, *proj_image.shape[::-1]), BF16),
                pltpu.VMEM((heads, 2, *proj_image.shape[::-1]), BF16),
                pltpu.VMEM((local_rows, size), BF16),
                pltpu.VMEM((nz, local_rows, 2 * size), BF16),
                pltpu.VMEM((local_rows, 128), F32),
                pltpu.VMEM((local_rows, 128), F32),
                pltpu.VMEM((local_rows, size), F32),
                pltpu.VMEM((heads, local_rows, size), BF16),
                pltpu.SMEM((1,), jnp.int32),
                pltpu.SMEM((1,), jnp.int32),
                dma((11,)),
                dma((2, 2, mod_weight.shape[1] // 128)),
                *pair(1),
                *pair(2, half, 2),
                *pair(2, half),
                *pair(2, half, 2),
                *pair(1),
                *pair(1),
                *pair(2, half, 2),
                *pair(1),
                *pair(1),
                *pair(2, half, 4),
                *pair(2, nx // 2, 2),
                *pair(2, nx // 2 + 1, 2),
            ],
            compiler_params=pltpu.CompilerParams(
                collective_id=0, has_side_effects=True, vmem_limit_bytes=56 * 1024 * 1024
            ),
        )(
            text_length,
            timestep,
            image_tokens,
            text_tokens,
            time_table,
            mod_weight,
            gains,
            qkv_image,
            qkv_text,
            proj_image.T,
            proj_text.T,
        )
        image_turned, text_out = pl.pallas_call(
            hand_out,
            out_shape=tuple(jax.ShapeDtypeStruct(r.shape, r.dtype) for r in results),
            in_specs=[vmem] * 2,
            out_specs=(vmem, vmem),
        )(*results)
        return image_turned.T, text_out

    return jax.shard_map(
        body,
        mesh=mesh,
        in_specs=(
            P(("groups", "seq"), None),
            P(("groups", "seq"), None),
            P("groups"),
            P("groups"),
            P(),
            P("seq", ("tensor", "sub")),
            P("seq", ("tensor", "sub")),
            P("seq", ("tensor", "sub")),
            P(None, None, ("tensor", "sub"), None),
            P(("tensor", "sub"), "seq"),
            P(("tensor", "sub"), "seq"),
        ),
        out_specs=(
            P(("groups", "seq"), ("tensor", "sub")),
            P(("groups", "seq"), ("tensor", "sub")),
        ),
        check_vma=False,
    )
```

```python
import functools
import math

import jax
import jax.numpy as jnp
from jax import lax
from jax.experimental import pallas as pl
from jax.experimental.pallas import tpu as pltpu
from jax.sharding import PartitionSpec as P

EPSILON = 1e-06
MESH = pl.DeviceIdType.MESH
BF16 = jnp.bfloat16
F32 = jnp.float32
RIGHT, LEFT = 0, 1


def rows_at(start, size, unit=16):
    if isinstance(start, int):
        return pl.ds(start, size)
    return pl.ds(pl.multiple_of(start, unit), size)


def kernel(
    sizes,
    paired,
    length_hbm,
    step_hbm,
    image_hbm,
    text_hbm,
    table_hbm,
    mod_hbm,
    gain_hbm,
    qkv_image,
    qkv_text,
    proj_image,
    proj_text,
    image_out,
    text_out,
    image_tokens,
    text_tokens,
    time_table,
    mod_weight,
    norm_gain,
    mod_rows,
    mod_in,
    mod_all,
    mean_of,
    rstd_of,
    hidden_image,
    hidden_text,
    weights,
    text_weights,
    sum_image,
    sum_text,
    text_qkv,
    proj_z,
    proj_all,
    query,
    key_value,
    row_max,
    row_sum,
    mixed,
    attended,
    text_length,
    timestep,
    load_sem,
    mod_sems,
    *pairs,
):
    nz, nx, nc = sizes
    (
        modx_sems,
        w_sems,
        wy_sems,
        t_sems,
        th_sems,
        tq_sems,
        p_sems,
        py_sems,
        px_sems,
        kv_sems,
        ax_sems,
        as_sems,
    ) = zip(pairs[0::2], pairs[1::2])
    heads = nx * nc
    z = lax.axis_index("seq")
    x = lax.axis_index("tensor")
    c = lax.axis_index("sub")
    me = x * nc + c
    own = lax.rem(lax.axis_index("groups"), 2) if paired else 0
    other_group = lax.axis_index("groups") + 1 - 2 * own if paired else 0
    image_rows, width = image_tokens.shape
    text_rows = text_tokens.shape[0]
    local_rows = image_rows + text_rows
    slab = qkv_image.shape[0]
    columns = qkv_image.shape[1]
    size = columns // 3
    active = c == own

    def when_active(run):
        if paired:
            pl.when(active)(run)
        else:
            run()


    def wrap(i, n):
        return lax.rem(i + n, n)

    def copy_of(src, dst, sems, index, device):
        return pltpu.make_async_remote_copy(
            src_ref=src,
            dst_ref=dst,
            send_sem=sems[0].at[0],
            recv_sem=sems[1].at[index],
            device_id=device,
            device_id_type=MESH,
        )

    def send(src, dst, sems, index, device):
        copy_of(src, dst, sems, index, device).start()

    def arrive(ref, sems, index, device):
        copy_of(ref, ref, sems, index, device).wait_recv()

    def sent(ref, sems, index, device):
        copy_of(ref, ref, sems, index, device).wait_send()

    right, left = {"seq": wrap(z + 1, nz)}, {"seq": wrap(z - 1, nz)}
    partner = {"groups": other_group}
    sibling = {"sub": 1 - c}

    barrier = pltpu.get_barrier_semaphore()
    peers = [{"seq": wrap(z + i, nz)} for i in range(1, nz)]
    plane = [
        {"tensor": lax.div(wrap(me + i, heads), nc), "sub": lax.rem(wrap(me + i, heads), nc)}
        for i in range(1, heads)
    ]
    far_first = sorted(range(1, nz), key=lambda i: -min(i, nz - i))
    greeted = [peers[i - 1] for i in far_first] + plane + ([partner] if paired else [])
    for device in greeted:
        pl.semaphore_signal(barrier, inc=1, device_id=device, device_id_type=MESH)

    piece = 2 * slab
    table_window = pl.ds(pl.multiple_of(lax.div(z, 2) * piece, 128), piece)
    loads = [
        pltpu.make_async_copy(src, dst, load_sem.at[i])
        for i, (src, dst) in enumerate(
            (
                (step_hbm, timestep),
                (length_hbm, text_length),
                (table_hbm.at[:, table_window], time_table),
                (mod_hbm, mod_weight),
                (qkv_image, weights.at[rows_at(z * slab, slab), :]),
                (qkv_text, text_weights.at[rows_at(z * slab, slab), :]),
                (proj_image, proj_z.at[z, 0]),
                (proj_text, proj_z.at[z, 1]),
                (text_hbm, text_tokens),
                (image_hbm, image_tokens),
                (gain_hbm, norm_gain),
            )
        )
    ]
    for copy in loads:
        copy.start()
    for copy in loads[:8]:
        copy.wait()

    picked = lax.broadcasted_iota(jnp.int32, time_table.shape, 0) == timestep[0]
    embedded = jnp.sum(
        jnp.where(picked, time_table[...].astype(F32), 0.0), axis=0, keepdims=True
    )
    vector = (embedded / (1.0 + jnp.exp(-embedded))).astype(BF16)
    vector_rows = jnp.where(lax.rem(z, 2) == 0, vector[:, :slab], vector[:, slab:])
    partial_sum = jnp.dot(vector_rows, mod_weight[...], preferred_element_type=F32)
    chunks = partial_sum.shape[1] // 128
    for i in range(chunks):
        mod_rows[i] = partial_sum[:, i * 128 : (i + 1) * 128]

    chunk = 16

    def statistics(tokens, first, last, at):
        def one(i, carry):
            rows = rows_at(i * chunk, chunk)
            values = tokens[rows, :].astype(F32)
            center = jnp.mean(values, axis=-1, keepdims=True)
            spread = jnp.mean(jnp.square(values - center), axis=-1, keepdims=True)
            out = rows_at(at + i * chunk, chunk)
            mean_of[out, :] = jnp.broadcast_to(center, (chunk, 128))
            rstd_of[out, :] = jnp.broadcast_to(lax.rsqrt(spread + EPSILON), (chunk, 128))
            return carry

        lax.fori_loop(first // chunk, last // chunk, one, 0)

    pl.semaphore_wait(barrier, len(greeted))

    def is_owner(i):
        return z == i % nz

    def mod_copy(i, src, dst, stage, device):
        return pltpu.make_async_remote_copy(
            src_ref=src,
            dst_ref=dst,
            send_sem=mod_sems.at[0, stage, i],
            recv_sem=mod_sems.at[1, stage, i],
            device_id=device,
            device_id_type=MESH,
        )

    def mod_total(i):
        return mod_all.at[me, :, pl.ds(i * 128, 128)]

    def mod_partial():
        for i in range(chunks):

            @pl.when(jnp.logical_not(is_owner(i)))
            def _():
                mod_copy(i, mod_rows.at[i], mod_in.at[i, z], 0, {"seq": i % nz}).start()

            @pl.when(is_owner(i))
            def _():
                mod_in[i, z] = mod_rows[i]

    def mod_reduce():
        for i in range(chunks):
            others = mod_in.at[i, pl.ds(0, nz - 1)]

            @pl.when(is_owner(i))
            def _():
                mod_copy(i, others, others, 0, right).wait_recv()
                total = mod_in[i, 0]
                for k in range(1, nz):
                    total = total + mod_in[i, k]
                mod_all[me, :, i * 128 : (i + 1) * 128] = total
                for device in peers:
                    mod_copy(i, mod_total(i), mod_total(i), 1, device).start()

    def mod_sent():
        for i in range(chunks):
            others = mod_in.at[i, pl.ds(0, nz - 1)]

            @pl.when(jnp.logical_not(is_owner(i)))
            def _():
                mod_copy(i, mod_rows.at[i], mod_rows.at[i], 0, right).wait_send()

            @pl.when(is_owner(i))
            def _():
                mod_copy(i, others, others, 1, right).wait_send()

    mod_partial()

    half = nz // 2

    def slab_of(way, d):
        return wrap(z - d, nz) if way == RIGHT else wrap(z + d, nz)

    def carried(way, d, part, parts):
        return d < half or (part < parts // 2) == (way == RIGHT)

    def ring_part(d, part, parts, part_ref, sems):
        for way, to in ((RIGHT, right), (LEFT, left)):
            if not carried(way, d, part, parts):
                continue
            here = part_ref(slab_of(way, d), part)
            if d > 0:
                arrive(here, sems, (way, d - 1, part), to)
            if d < half and carried(way, d + 1, part, parts):
                send(here, here, sems, (way, d, part), to)

    share = slab // 2 if paired else slab

    def w_part(block, part):
        start = block * slab + own * share + part * (share // 2)
        return weights.at[rows_at(start, share // 2), :]

    def y_part(block, part, of):
        start = block * slab + of * share + part * (share // 2)
        return weights.at[rows_at(start, share // 2), :]

    def t_part(block, part):
        return text_weights.at[rows_at(block * slab + part * (slab // 2), slab // 2), :]

    def p_part(block, part):
        return proj_z.at[block, :, rows_at(own * share + part * (share // 2), share // 2), :]

    def p_share(ref, block):
        return ref.at[block, :, rows_at(own * share, share), :]

    def weight_step(d, tasks=((), ())):
        for part in (0, 1):
            ring_part(d, part, 2, w_part, w_sems)
            if paired and d > 0:
                for way in (RIGHT, LEFT):
                    if carried(way, d, part, 2):
                        here = y_part(slab_of(way, d), part, own)
                        send(here, here, wy_sems, (way, d - 1, part), partner)
            when_active(lambda: ring_part(d, part, 2, t_part, t_sems))
            for task in tasks[part]:
                task()

    def weight_wait(d):
        if paired:
            for part in (0, 1):
                for way in (RIGHT, LEFT):
                    if carried(way, d, part, 2):
                        here = y_part(slab_of(way, d), part, 1 - own)
                        arrive(here, wy_sems, (way, d - 1, part), partner)

    weight_step(0)

    for copy in loads[8:]:
        copy.wait()
    statistics(text_tokens, 0, text_rows, image_rows)
    statistics(image_tokens, 0, image_rows // 2, 0)

    def mod_over_seq():
        for i in range(chunks):

            @pl.when(jnp.logical_not(is_owner(i)))
            def _():
                mod_copy(i, mod_total(i), mod_total(i), 1, right).wait_recv()

        for device in plane:
            send(mod_all.at[me], mod_all.at[me], modx_sems, (0,), device)

    def mod_over_plane():
        arrive(mod_all.at[pl.ds(0, heads - 1)], modx_sems, (0,), sibling)

    per_block = mod_weight.shape[1] // piece
    pieces = width // piece

    def mod_piece(index):
        if isinstance(index, int):
            return mod_all[index // per_block, :, pl.ds(index % per_block * piece, piece)]
        offset = pl.multiple_of(lax.rem(index, per_block) * piece, 128)
        return mod_all[lax.div(index, per_block), :, pl.ds(offset, piece)]

    def hide(tokens, hidden, stream, first, last, at):
        def one(i, carry):
            rows = rows_at(i * chunk, chunk)
            out = rows_at(at + i * chunk, chunk)
            center, scale = mean_of[out, 0:1], rstd_of[out, 0:1]
            for p in range(pieces):
                shift = mod_piece((stream * 3) * pieces + p)
                scaling = mod_piece((stream * 3 + 1) * pieces + p)
                values = tokens[rows, p * piece : (p + 1) * piece].astype(F32)
                values = ((values - center) * scale * (1.0 + scaling) + shift).astype(BF16)
                hidden[rows, p * piece : (p + 1) * piece] = values
            return carry

        lax.fori_loop(first // chunk, last // chunk, one, 0)

    sum_image[...] = jnp.zeros_like(sum_image)
    sum_text[...] = jnp.zeros_like(sum_text)
    depth = 4 * slab

    def block_at(j):
        step = lax.div(j + 1, 2)
        return wrap(jnp.where(lax.rem(j, 2) == 1, z - step, z + step), nz)

    pieces_of_depth = nz * slab // depth
    first_piece = lax.div(z * slab, depth)
    order = [i for i in range(pieces_of_depth) if i != pieces_of_depth // 2]
    order += [pieces_of_depth // 2]

    def project(hidden, total, shards, which):
        for i in which:
            index = lax.rem(first_piece + i, pieces_of_depth)
            at = pl.ds(pl.multiple_of(index * depth, 128), depth)
            total[...] += jnp.dot(hidden[:, at], shards[at, :], preferred_element_type=F32)

    def give_block(block):
        target = {"tensor": lax.div(block, nc), "sub": lax.rem(block, nc)}

        @pl.when(block != me)
        def _():
            send(p_share(proj_z, block), p_share(proj_all, me), px_sems, (0,), target)

        @pl.when(block == me)
        def _():
            rows = rows_at(own * share, share)
            proj_all[me, :, rows, :] = proj_z[block, :, rows, :]

    def proj_step(d):
        for part in (0, 1):
            ring_part(d, part, 2, p_part, p_sems)
        give_block(slab_of(RIGHT, d))
        if 0 < d < half:
            give_block(slab_of(LEFT, d))

    away = lax.rem(z - me + nz, nz)
    away = jnp.minimum(away, nz - away)
    all_shares = proj_all.at[:, :, rows_at(own * share, share), :]
    other_shares = proj_all.at[:, :, rows_at((1 - own) * share, share), :]

    def hand_over(d):
        @pl.when(away == d)
        def _():
            arrive(proj_all.at[pl.ds(0, heads - 1), :, pl.ds(0, share), :], px_sems, (0,), sibling)
            if paired:
                send(all_shares, all_shares, py_sems, (0,), partner)

    lag = min(5, half)
    proj_plan = {}
    for d in range(half + 1):
        proj_plan.setdefault(lag + d, []).append((proj_step, d))
        after = max(lag + d + 3, half + 1 + (d + 1) // 2)
        proj_plan.setdefault(min(after, 2 * half + 1), []).append((hand_over, d))

    def proj_advance(step):
        for call, d in proj_plan.get(step, ()):
            call(d)

    def hidden_exchange():
        if paired:

            @pl.when(jnp.logical_not(active))
            def _():
                send(both[0], both[1], th_sems, (0,), partner)

    both = (
        hidden_text.at[pl.ds(0, text_rows), :],
        hidden_text.at[pl.ds(text_rows, text_rows), :],
    )
    middle = image_rows // 2

    def stats_of(first):
        return lambda: statistics(image_tokens, first, first + middle // 2, 0)

    def hide_of(first):
        return lambda: hide(image_tokens, hidden_image, 0, first, first + middle // 2, 0)

    def hide_text():
        mod_over_plane()
        hide(text_tokens, hidden_text, 1, 0, text_rows, image_rows)
        hidden_exchange()

    quarter_rows = middle // 2
    early = [
        (1, 0, stats_of(middle)),
        (1, 1, stats_of(middle + quarter_rows)),
        (2, 1, mod_reduce),
        (4, 1, mod_over_seq),
        (6, 0, hide_text),
        (6, 1, hide_of(0)),
        (7, 0, hide_of(quarter_rows)),
        (7, 1, hide_of(middle)),
        (8, 1, hide_of(middle + quarter_rows)),
    ]
    for d in range(1, half + 1):
        tasks = [
            [task for at, place, task in early if (min(at, half), place if at < half else 1) == (d, p)]
            if d < half or p == 1
            else []
            for p in (0, 1)
        ]
        weight_step(d, tasks)
        proj_advance(d)
        if d > 2:
            weight_wait(d - 2)
    if half > 1:
        weight_wait(half - 1)
    project(hidden_image, sum_image, weights, order[:-1])
    weight_wait(half)
    project(hidden_image, sum_image, weights, order[-1:])

    def normed(values, gain):
        return (
            values
            * lax.rsqrt(jnp.mean(values * values, axis=-1, keepdims=True) + EPSILON)
            * gain
        ).astype(BF16)

    def normed_three(total, stream):
        return (
            normed(total[:, 0:size], norm_gain[stream, 0]),
            normed(total[:, size : 2 * size], norm_gain[stream, 1]),
            total[:, 2 * size : 3 * size].astype(BF16),
        )

    quarter = local_rows // 64 * 16
    starts = (0, local_rows // 2 - quarter, local_rows // 2, local_rows - quarter, local_rows)

    def kv_part(block, part):
        return key_value.at[block, pl.ds(starts[part], starts[part + 1] - starts[part]), :]

    q, k, v = normed_three(sum_image[...], 0)
    query[0:image_rows, :] = q
    key_value[z, 0:image_rows, 0:size] = k
    key_value[z, 0:image_rows, size : 2 * size] = v
    for part in (0, 1, 2):
        ring_part(0, part, 4, kv_part, kv_sems)

    def text_projection():
        if paired:
            arrive(both[1], th_sems, (0,), partner)
        project(hidden_text, sum_text, text_weights, order)
        for side in (0, 1) if paired else (0,):
            parts = normed_three(sum_text[side * text_rows : (side + 1) * text_rows, :], 1)
            for i in range(3):
                text_qkv[side, :, i * size : (i + 1) * size] = parts[i]
        if paired:
            send(text_qkv.at[1], text_qkv.at[0], tq_sems, (0,), partner)

    when_active(text_projection)
    if paired:

        @pl.when(jnp.logical_not(active))
        def _():
            arrive(text_qkv.at[0], tq_sems, (0,), partner)

    query[image_rows:, :] = text_qkv[0, :, 0:size]
    key_value[z, image_rows:, :] = text_qkv[0, :, size : 3 * size]
    ring_part(0, 3, 4, kv_part, kv_sems)

    row_max[...] = jnp.full_like(row_max, -1e30)
    row_sum[...] = jnp.zeros_like(row_sum)
    mixed[...] = jnp.zeros_like(mixed)
    factor = float(size) ** (-0.5) * math.log2(math.e)

    def attend(first, last):
        def one(j, carry):
            block = block_at(j)
            scores = lax.dot_general(
                query[...],
                key_value[block, :, 0:size],
                (((1,), (1,)), ((), ())),
                preferred_element_type=F32,
            )
            within = lax.broadcasted_iota(jnp.int32, scores.shape, 1)
            slot = block * text_rows + within - image_rows
            usable = (within < image_rows) | (slot < text_length[0])
            scores = jnp.where(usable, scores, -1e30)
            old = row_max[:, 0:1]
            new = jnp.maximum(old, jnp.max(scores, axis=-1, keepdims=True))
            probs = jnp.exp2((scores - new) * factor)
            fade = jnp.exp2((old - new) * factor)
            row_max[...] = jnp.broadcast_to(new, row_max.shape)
            total = row_sum[:, 0:1] * fade + jnp.sum(probs, axis=-1, keepdims=True)
            row_sum[...] = jnp.broadcast_to(total, row_sum.shape)
            mixed[...] = mixed[...] * fade + jnp.dot(
                probs.astype(BF16),
                key_value[block, :, size : 2 * size],
                preferred_element_type=F32,
            )
            return carry

        lax.fori_loop(first, last, one, 0)

    for d in range(1, half + 1):
        for part in (0, 1):
            ring_part(d, part, 4, kv_part, kv_sems)
        attend(max(2 * d - 3, 0), 2 * d - 2 if d > 1 else 1)
        for part in (2, 3):
            ring_part(d, part, 4, kv_part, kv_sems)
        proj_advance(half + d)
        if d > 1:
            attend(2 * d - 2, 2 * d - 1)
    proj_advance(2 * half + 1)
    attend(nz - 1, nz)

    attended[me] = (mixed[...] / row_sum[:, 0:1]).astype(BF16)

    x_half = nx // 2
    x_right, x_left = {"tensor": wrap(x + 1, nx)}, {"tensor": wrap(x - 1, nx)}
    half_rows = local_rows // 2

    def x_carried(way, d, part):
        return d < x_half or (part == 0) == (way == RIGHT)

    def x_block(way, d):
        return (wrap(x - d, nx) if way == RIGHT else wrap(x + d, nx)) * nc + c

    def a_part(block, part):
        return attended.at[block, pl.ds(part * half_rows, half_rows), :]

    for d in range(0, x_half + 1):
        for part in (0, 1):
            for way, to in ((RIGHT, x_right), (LEFT, x_left)):
                if not x_carried(way, d, part):
                    continue
                here = a_part(x_block(way, d), part)
                if d > 0:
                    arrive(here, ax_sems, (way, d - 1, part), to)
                if d < x_half and x_carried(way, d + 1, part):
                    send(here, here, ax_sems, (way, d, part), to)
                if d > 0 or way == RIGHT:
                    send(here, here, as_sems, (way, d, part), sibling)

    if paired:
        arrive(other_shares, py_sems, (0,), partner)

    across = 1 - 2 * c
    for d in range(0, x_half + 1):
        for part in (0, 1):
            for way in (RIGHT, LEFT):
                if x_carried(way, d, part) and (d > 0 or way == RIGHT):
                    arrive(
                        a_part(x_block(way, d) + across, part), as_sems, (way, d, part), sibling
                    )

    out_width = text_out.shape[1]
    image_sum, text_sum = None, None
    for h in range(0, heads, 2):
        rows = jnp.concatenate([attended[h], attended[h + 1]], axis=1)
        image_w = jnp.concatenate([proj_all[h, 0], proj_all[h + 1, 0]], axis=1)
        text_w = jnp.concatenate([proj_all[h, 1], proj_all[h + 1, 1]], axis=1)
        turned = (((1,), (1,)), ((), ()))
        image_term = lax.dot_general(
            rows[:image_rows], image_w, turned, preferred_element_type=F32
        )
        text_term = lax.dot_general(rows[image_rows:], text_w, turned, preferred_element_type=F32)
        image_sum = image_term if image_sum is None else image_sum + image_term
        text_sum = text_term if text_sum is None else text_sum + text_term

    def own_columns(wide):
        return jnp.where(c == 0, wide[:, :out_width], wide[:, out_width:])

    window = pl.ds(pl.multiple_of(x * 2 * out_width, 128), 2 * out_width)
    for tokens, total, out, stream in (
        (image_tokens, image_sum, image_out, 0),
        (text_tokens, text_sum, text_out, 1),
    ):
        gate = own_columns(mod_piece((stream * 3 + 2) * pieces + x))
        base = own_columns(tokens[:, window].astype(F32))
        result = base + gate * total
        out[...] = (jnp.transpose(result) if stream == 0 else result).astype(BF16)

    mod_sent()
    sent(mod_all.at[pl.ds(0, heads - 1)], modx_sems, (0,), sibling)
    blocks = pl.ds(0, nz - 1)
    sent(weights.at[pl.ds(0, (nz - 1) * share), :], w_sems, (0, 0, 0), right)
    sent(proj_z.at[blocks, :, pl.ds(0, share), :], p_sems, (0, 0, 0), right)
    sent(proj_all.at[pl.ds(0, heads - 1), :, pl.ds(0, share), :], px_sems, (0,), sibling)
    sent(key_value.at[blocks], kv_sems, (0, 0, 0), right)
    sent(attended.at[pl.ds(0, nx - 1)], ax_sems, (0, 0, 0), x_right)
    sent(attended.at[pl.ds(0, nx)], as_sems, (0, 0, 0), sibling)
    if paired:
        sent(weights.at[pl.ds(0, (nz - 1) * share), :], wy_sems, (0, 0, 0), partner)
        sent(all_shares, py_sems, (0,), partner)

    def text_sent():
        sent(text_weights.at[pl.ds(0, (nz - 1) * slab), :], t_sems, (0, 0, 0), right)
        if paired:
            sent(text_qkv.at[1], tq_sems, (0,), partner)

    when_active(text_sent)
    if paired:

        @pl.when(jnp.logical_not(active))
        def _():
            sent(both[0], th_sems, (0,), partner)


def hand_out(image, text, image_out, text_out):
    image_out[...] = image[...]
    text_out[...] = text[...]


def solution(mesh):
    nz, nx, nc = mesh.shape["seq"], mesh.shape["tensor"], mesh.shape["sub"]
    paired = mesh.shape["groups"] % 2 == 0
    heads = nx * nc

    def body(
        image_tokens,
        text_tokens,
        timestep,
        text_length,
        time_table,
        mod_weight,
        qkv_image,
        qkv_text,
        norm_gain,
        proj_image,
        proj_text,
    ):
        slab = qkv_image.shape[0]
        gains = norm_gain.reshape(2, 2, 1, norm_gain.shape[-1])
        image_rows, width = image_tokens.shape
        text_rows = text_tokens.shape[0]
        local_rows = image_rows + text_rows
        columns = qkv_image.shape[1]
        size = columns // 3
        out_width = width // heads
        half = nz // 2
        vmem = pl.BlockSpec(memory_space=pltpu.VMEM)
        anywhere = pl.BlockSpec(memory_space=pl.ANY)
        dma = pltpu.SemaphoreType.DMA

        def pair(*shape):
            return dma((1,)), dma(shape)

        results = pl.pallas_call(
            functools.partial(kernel, (nz, nx, nc), paired),
            out_shape=(
                jax.ShapeDtypeStruct((out_width, image_rows), BF16),
                jax.ShapeDtypeStruct((text_rows, out_width), BF16),
            ),
            in_specs=[pl.BlockSpec(memory_space=pltpu.HBM)] * 2 + [anywhere] * 9,
            out_specs=(vmem, vmem),
            scratch_shapes=[
                pltpu.VMEM(image_tokens.shape, BF16),
                pltpu.VMEM(text_tokens.shape, BF16),
                pltpu.VMEM((time_table.shape[0], 2 * slab), BF16),
                pltpu.VMEM(mod_weight.shape, BF16),
                pltpu.VMEM(gains.shape, F32),
                pltpu.VMEM((mod_weight.shape[1] // 128, 1, 128), F32),
                pltpu.VMEM((mod_weight.shape[1] // 128, nz, 1, 128), F32),
                pltpu.VMEM((heads, 1, mod_weight.shape[1]), F32),
                pltpu.VMEM((local_rows, 128), F32),
                pltpu.VMEM((local_rows, 128), F32),
                pltpu.VMEM((image_rows, width), BF16),
                pltpu.VMEM((2 * text_rows, width), BF16),
                pltpu.VMEM((width, columns), BF16),
                pltpu.VMEM((width, columns), BF16),
                pltpu.VMEM((image_rows, columns), F32),
                pltpu.VMEM((2 * text_rows, columns), F32),
                pltpu.VMEM((2, text_rows, columns), BF16),
                pltpu.VMEM((nz, 2, *proj_image.shape[::-1]), BF16),
                pltpu.VMEM((heads, 2, *proj_image.shape[::-1]), BF16),
                pltpu.VMEM((local_rows, size), BF16),
                pltpu.VMEM((nz, local_rows, 2 * size), BF16),
                pltpu.VMEM((local_rows, 128), F32),
                pltpu.VMEM((local_rows, 128), F32),
                pltpu.VMEM((local_rows, size), F32),
                pltpu.VMEM((heads, local_rows, size), BF16),
                pltpu.SMEM((1,), jnp.int32),
                pltpu.SMEM((1,), jnp.int32),
                dma((11,)),
                dma((2, 2, mod_weight.shape[1] // 128)),
                *pair(1),
                *pair(2, half, 2),
                *pair(2, half, 2),
                *pair(2, half, 2),
                *pair(1),
                *pair(1),
                *pair(2, half, 2),
                *pair(1),
                *pair(1),
                *pair(2, half, 4),
                *pair(2, nx // 2, 2),
                *pair(2, nx // 2 + 1, 2),
            ],
            compiler_params=pltpu.CompilerParams(
                collective_id=0, has_side_effects=True, vmem_limit_bytes=56 * 1024 * 1024
            ),
        )(
            text_length,
            timestep,
            image_tokens,
            text_tokens,
            time_table,
            mod_weight,
            gains,
            qkv_image,
            qkv_text,
            proj_image.T,
            proj_text.T,
        )
        image_turned, text_out = pl.pallas_call(
            hand_out,
            out_shape=tuple(jax.ShapeDtypeStruct(r.shape, r.dtype) for r in results),
            in_specs=[vmem] * 2,
            out_specs=(vmem, vmem),
        )(*results)
        return image_turned.T, text_out

    return jax.shard_map(
        body,
        mesh=mesh,
        in_specs=(
            P(("groups", "seq"), None),
            P(("groups", "seq"), None),
            P("groups"),
            P("groups"),
            P(),
            P("seq", ("tensor", "sub")),
            P("seq", ("tensor", "sub")),
            P("seq", ("tensor", "sub")),
            P(None, None, ("tensor", "sub"), None),
            P(("tensor", "sub"), "seq"),
            P(("tensor", "sub"), "seq"),
        ),
        out_specs=(
            P(("groups", "seq"), ("tensor", "sub")),
            P(("groups", "seq"), ("tensor", "sub")),
        ),
        check_vma=False,
    )
```

```python
import functools
import math

import jax
import jax.numpy as jnp
from jax import lax
from jax.experimental import pallas as pl
from jax.experimental.pallas import tpu as pltpu
from jax.sharding import PartitionSpec as P

EPSILON = 1e-06
MESH = pl.DeviceIdType.MESH
BF16 = jnp.bfloat16
F32 = jnp.float32
RIGHT, LEFT = 0, 1


def rows_at(start, size, unit=16):
    if isinstance(start, int):
        return pl.ds(start, size)
    return pl.ds(pl.multiple_of(start, unit), size)


def kernel(
    sizes,
    paired,
    length_hbm,
    step_hbm,
    image_hbm,
    text_hbm,
    table_hbm,
    mod_hbm,
    gain_hbm,
    qkv_image,
    qkv_text,
    proj_image,
    proj_text,
    image_out,
    text_out,
    image_tokens,
    text_tokens,
    time_table,
    mod_weight,
    norm_gain,
    mod_rows,
    mod_in,
    mod_all,
    mean_of,
    rstd_of,
    hidden_image,
    hidden_text,
    weights,
    text_weights,
    sum_image,
    sum_text,
    text_qkv,
    proj_z,
    proj_all,
    query,
    key_value,
    row_max,
    row_sum,
    mixed,
    attended,
    text_length,
    timestep,
    load_sem,
    mod_sems,
    *pairs,
):
    nz, nx, nc = sizes
    (
        modx_sems,
        w_sems,
        wy_sems,
        t_sems,
        th_sems,
        tq_sems,
        p_sems,
        py_sems,
        px_sems,
        kv_sems,
        ax_sems,
        as_sems,
    ) = zip(pairs[0::2], pairs[1::2])
    heads = nx * nc
    z = lax.axis_index("seq")
    x = lax.axis_index("tensor")
    c = lax.axis_index("sub")
    me = x * nc + c
    own = lax.rem(lax.axis_index("groups"), 2) if paired else 0
    other_group = lax.axis_index("groups") + 1 - 2 * own if paired else 0
    image_rows, width = image_tokens.shape
    text_rows = text_tokens.shape[0]
    local_rows = image_rows + text_rows
    slab = qkv_image.shape[0]
    columns = qkv_image.shape[1]
    size = columns // 3
    active = c == own

    def when_active(run):
        if paired:
            pl.when(active)(run)
        else:
            run()


    def wrap(i, n):
        return lax.rem(i + n, n)

    def copy_of(src, dst, sems, index, device):
        return pltpu.make_async_remote_copy(
            src_ref=src,
            dst_ref=dst,
            send_sem=sems[0].at[0],
            recv_sem=sems[1].at[index],
            device_id=device,
            device_id_type=MESH,
        )

    def send(src, dst, sems, index, device):
        copy_of(src, dst, sems, index, device).start()

    def arrive(ref, sems, index, device):
        copy_of(ref, ref, sems, index, device).wait_recv()

    def sent(ref, sems, index, device):
        copy_of(ref, ref, sems, index, device).wait_send()

    right, left = {"seq": wrap(z + 1, nz)}, {"seq": wrap(z - 1, nz)}
    partner = {"groups": other_group}
    sibling = {"sub": 1 - c}

    barrier = pltpu.get_barrier_semaphore()
    peers = [{"seq": wrap(z + i, nz)} for i in range(1, nz)]
    plane = [
        {"tensor": lax.div(wrap(me + i, heads), nc), "sub": lax.rem(wrap(me + i, heads), nc)}
        for i in range(1, heads)
    ]
    far_first = sorted(range(1, nz), key=lambda i: -min(i, nz - i))
    greeted = [peers[i - 1] for i in far_first] + plane + ([partner] if paired else [])
    for device in greeted:
        pl.semaphore_signal(barrier, inc=1, device_id=device, device_id_type=MESH)

    piece = 2 * slab
    table_window = pl.ds(pl.multiple_of(lax.div(z, 2) * piece, 128), piece)
    loads = [
        pltpu.make_async_copy(src, dst, load_sem.at[i])
        for i, (src, dst) in enumerate(
            (
                (step_hbm, timestep),
                (length_hbm, text_length),
                (table_hbm.at[:, table_window], time_table),
                (mod_hbm, mod_weight),
                (qkv_image, weights.at[rows_at(z * slab, slab), :]),
                (qkv_text, text_weights.at[rows_at(z * slab, slab), :]),
                (proj_image, proj_z.at[z, 0]),
                (proj_text, proj_z.at[z, 1]),
                (text_hbm, text_tokens),
                (image_hbm, image_tokens),
                (gain_hbm, norm_gain),
            )
        )
    ]
    for copy in loads:
        copy.start()
    for copy in loads[:8]:
        copy.wait()

    picked = lax.broadcasted_iota(jnp.int32, time_table.shape, 0) == timestep[0]
    embedded = jnp.sum(
        jnp.where(picked, time_table[...].astype(F32), 0.0), axis=0, keepdims=True
    )
    vector = (embedded / (1.0 + jnp.exp(-embedded))).astype(BF16)
    vector_rows = jnp.where(lax.rem(z, 2) == 0, vector[:, :slab], vector[:, slab:])
    partial_sum = jnp.dot(vector_rows, mod_weight[...], preferred_element_type=F32)
    chunks = partial_sum.shape[1] // 128
    for i in range(chunks):
        mod_rows[i] = partial_sum[:, i * 128 : (i + 1) * 128]

    chunk = 16

    def statistics(tokens, first, last, at):
        def one(i, carry):
            rows = rows_at(i * chunk, chunk)
            values = tokens[rows, :].astype(F32)
            center = jnp.mean(values, axis=-1, keepdims=True)
            spread = jnp.mean(jnp.square(values - center), axis=-1, keepdims=True)
            out = rows_at(at + i * chunk, chunk)
            mean_of[out, :] = jnp.broadcast_to(center, (chunk, 128))
            rstd_of[out, :] = jnp.broadcast_to(lax.rsqrt(spread + EPSILON), (chunk, 128))
            return carry

        lax.fori_loop(first // chunk, last // chunk, one, 0)

    pl.semaphore_wait(barrier, len(greeted))

    def is_owner(i):
        return z == i % nz

    def mod_copy(i, src, dst, stage, device):
        return pltpu.make_async_remote_copy(
            src_ref=src,
            dst_ref=dst,
            send_sem=mod_sems.at[0, stage, i],
            recv_sem=mod_sems.at[1, stage, i],
            device_id=device,
            device_id_type=MESH,
        )

    def mod_total(i):
        return mod_all.at[me, :, pl.ds(i * 128, 128)]

    def mod_partial():
        for i in range(chunks):

            @pl.when(jnp.logical_not(is_owner(i)))
            def _():
                mod_copy(i, mod_rows.at[i], mod_in.at[i, z], 0, {"seq": i % nz}).start()

            @pl.when(is_owner(i))
            def _():
                mod_in[i, z] = mod_rows[i]

    def mod_reduce():
        for i in range(chunks):
            others = mod_in.at[i, pl.ds(0, nz - 1)]

            @pl.when(is_owner(i))
            def _():
                mod_copy(i, others, others, 0, right).wait_recv()
                total = mod_in[i, 0]
                for k in range(1, nz):
                    total = total + mod_in[i, k]
                mod_all[me, :, i * 128 : (i + 1) * 128] = total
                for device in peers:
                    mod_copy(i, mod_total(i), mod_total(i), 1, device).start()

    def mod_sent():
        for i in range(chunks):
            others = mod_in.at[i, pl.ds(0, nz - 1)]

            @pl.when(jnp.logical_not(is_owner(i)))
            def _():
                mod_copy(i, mod_rows.at[i], mod_rows.at[i], 0, right).wait_send()

            @pl.when(is_owner(i))
            def _():
                mod_copy(i, others, others, 1, right).wait_send()

    mod_partial()

    half = nz // 2

    def slab_of(way, d):
        return wrap(z - d, nz) if way == RIGHT else wrap(z + d, nz)

    def carried(way, d, part, parts):
        return d < half or (part < parts // 2) == (way == RIGHT)

    def ring_part(d, part, parts, part_ref, sems):
        for way, to in ((RIGHT, right), (LEFT, left)):
            if not carried(way, d, part, parts):
                continue
            here = part_ref(slab_of(way, d), part)
            if d > 0:
                arrive(here, sems, (way, d - 1, part), to)
            if d < half and carried(way, d + 1, part, parts):
                send(here, here, sems, (way, d, part), to)

    share = slab // 2 if paired else slab

    def w_part(block, part):
        start = block * slab + own * share + part * (share // 2)
        return weights.at[rows_at(start, share // 2), :]

    def y_part(block, part, of):
        start = block * slab + of * share + part * (share // 2)
        return weights.at[rows_at(start, share // 2), :]

    def t_part(block, part):
        return text_weights.at[rows_at(block * slab + part * (slab // 2), slab // 2), :]

    def p_part(block, part):
        return proj_z.at[block, :, rows_at(own * share + part * (share // 2), share // 2), :]

    def p_share(ref, block):
        return ref.at[block, :, rows_at(own * share, share), :]

    def weight_step(d, tasks=((), ())):
        for part in (0, 1):
            ring_part(d, part, 2, w_part, w_sems)
            if paired and d > 0:
                for way in (RIGHT, LEFT):
                    if carried(way, d, part, 2):
                        here = y_part(slab_of(way, d), part, own)
                        send(here, here, wy_sems, (way, d - 1, part), partner)
            when_active(lambda: ring_part(d, part, 2, t_part, t_sems))
            for task in tasks[part]:
                task()

    def weight_wait(d):
        if paired:
            for part in (0, 1):
                for way in (RIGHT, LEFT):
                    if carried(way, d, part, 2):
                        here = y_part(slab_of(way, d), part, 1 - own)
                        arrive(here, wy_sems, (way, d - 1, part), partner)

    weight_step(0)

    for copy in loads[8:]:
        copy.wait()
    statistics(text_tokens, 0, text_rows, image_rows)
    statistics(image_tokens, 0, image_rows // 2, 0)

    def mod_over_seq():
        for i in range(chunks):

            @pl.when(jnp.logical_not(is_owner(i)))
            def _():
                mod_copy(i, mod_total(i), mod_total(i), 1, right).wait_recv()

        for device in plane:
            send(mod_all.at[me], mod_all.at[me], modx_sems, (0,), device)

    def mod_over_plane():
        arrive(mod_all.at[pl.ds(0, heads - 1)], modx_sems, (0,), sibling)

    per_block = mod_weight.shape[1] // piece
    pieces = width // piece

    def mod_piece(index):
        if isinstance(index, int):
            return mod_all[index // per_block, :, pl.ds(index % per_block * piece, piece)]
        offset = pl.multiple_of(lax.rem(index, per_block) * piece, 128)
        return mod_all[lax.div(index, per_block), :, pl.ds(offset, piece)]

    def hide(tokens, hidden, stream, first, last, at):
        def one(i, carry):
            rows = rows_at(i * chunk, chunk)
            out = rows_at(at + i * chunk, chunk)
            center, scale = mean_of[out, 0:1], rstd_of[out, 0:1]
            for p in range(pieces):
                shift = mod_piece((stream * 3) * pieces + p)
                scaling = mod_piece((stream * 3 + 1) * pieces + p)
                values = tokens[rows, p * piece : (p + 1) * piece].astype(F32)
                values = ((values - center) * scale * (1.0 + scaling) + shift).astype(BF16)
                hidden[rows, p * piece : (p + 1) * piece] = values
            return carry

        lax.fori_loop(first // chunk, last // chunk, one, 0)

    sum_image[...] = jnp.zeros_like(sum_image)
    sum_text[...] = jnp.zeros_like(sum_text)
    depth = 4 * slab

    def block_at(j):
        step = lax.div(j + 1, 2)
        return wrap(jnp.where(lax.rem(j, 2) == 1, z - step, z + step), nz)

    pieces_of_depth = nz * slab // depth
    first_piece = lax.div(z * slab, depth)
    order = [i for i in range(pieces_of_depth) if i != pieces_of_depth // 2]
    order += [pieces_of_depth // 2]

    def project(hidden, total, shards, which):
        for i in which:
            index = lax.rem(first_piece + i, pieces_of_depth)
            at = pl.ds(pl.multiple_of(index * depth, 128), depth)
            total[...] += jnp.dot(hidden[:, at], shards[at, :], preferred_element_type=F32)

    def give_block(block):
        target = {"tensor": lax.div(block, nc), "sub": lax.rem(block, nc)}

        @pl.when(block != me)
        def _():
            send(p_share(proj_z, block), p_share(proj_all, me), px_sems, (0,), target)

        @pl.when(block == me)
        def _():
            rows = rows_at(own * share, share)
            proj_all[me, :, rows, :] = proj_z[block, :, rows, :]

    def proj_step(d):
        for part in (0, 1):
            ring_part(d, part, 2, p_part, p_sems)
        give_block(slab_of(RIGHT, d))
        if 0 < d < half:
            give_block(slab_of(LEFT, d))

    away = lax.rem(z - me + nz, nz)
    away = jnp.minimum(away, nz - away)
    all_shares = proj_all.at[:, :, rows_at(own * share, share), :]
    other_shares = proj_all.at[:, :, rows_at((1 - own) * share, share), :]

    def hand_over(d):
        @pl.when(away == d)
        def _():
            arrive(proj_all.at[pl.ds(0, heads - 1), :, pl.ds(0, share), :], px_sems, (0,), sibling)
            if paired:
                send(all_shares, all_shares, py_sems, (0,), partner)

    lag = min(5, half)
    proj_plan = {}
    for d in range(half + 1):
        proj_plan.setdefault(lag + d, []).append((proj_step, d))
        after = max(lag + d + 3, half + 1 + (d + 1) // 2)
        proj_plan.setdefault(min(after, 2 * half + 1), []).append((hand_over, d))

    def proj_advance(step):
        for call, d in proj_plan.get(step, ()):
            call(d)

    def hidden_exchange():
        if paired:

            @pl.when(jnp.logical_not(active))
            def _():
                send(both[0], both[1], th_sems, (0,), partner)

    both = (
        hidden_text.at[pl.ds(0, text_rows), :],
        hidden_text.at[pl.ds(text_rows, text_rows), :],
    )
    middle = image_rows // 2

    def stats_of(first):
        return lambda: statistics(image_tokens, first, first + middle // 2, 0)

    def hide_of(first):
        return lambda: hide(image_tokens, hidden_image, 0, first, first + middle // 2, 0)

    def hide_text():
        mod_over_plane()
        hide(text_tokens, hidden_text, 1, 0, text_rows, image_rows)
        hidden_exchange()

    quarter_rows = middle // 2
    early = [
        (1, 0, stats_of(middle)),
        (1, 1, stats_of(middle + quarter_rows)),
        (2, 1, mod_reduce),
        (4, 1, mod_over_seq),
        (6, 0, hide_text),
        (6, 1, hide_of(0)),
        (7, 0, hide_of(quarter_rows)),
        (7, 1, hide_of(middle)),
        (8, 1, hide_of(middle + quarter_rows)),
    ]
    for d in range(1, half + 1):
        tasks = [
            [task for at, place, task in early if (min(at, half), place if at < half else 1) == (d, p)]
            if d < half or p == 1
            else []
            for p in (0, 1)
        ]
        weight_step(d, tasks)
        proj_advance(d)
        if d > 2:
            weight_wait(d - 2)
    if half > 1:
        weight_wait(half - 1)
    project(hidden_image, sum_image, weights, order[:-1])
    weight_wait(half)
    project(hidden_image, sum_image, weights, order[-1:])

    def normed(values, gain):
        return (
            values
            * lax.rsqrt(jnp.mean(values * values, axis=-1, keepdims=True) + EPSILON)
            * gain
        ).astype(BF16)

    def normed_three(total, stream):
        return (
            normed(total[:, 0:size], norm_gain[stream, 0]),
            normed(total[:, size : 2 * size], norm_gain[stream, 1]),
            total[:, 2 * size : 3 * size].astype(BF16),
        )

    quarter = local_rows // 64 * 16
    starts = (0, local_rows // 2 - quarter, local_rows // 2, local_rows - quarter, local_rows)

    def kv_part(block, part):
        return key_value.at[block, pl.ds(starts[part], starts[part + 1] - starts[part]), :]

    q, k, v = normed_three(sum_image[...], 0)
    query[0:image_rows, :] = q
    key_value[z, 0:image_rows, 0:size] = k
    key_value[z, 0:image_rows, size : 2 * size] = v
    for part in (0, 1, 2):
        ring_part(0, part, 4, kv_part, kv_sems)

    def text_projection():
        if paired:
            arrive(both[1], th_sems, (0,), partner)
        project(hidden_text, sum_text, text_weights, order)
        for side in (0, 1) if paired else (0,):
            parts = normed_three(sum_text[side * text_rows : (side + 1) * text_rows, :], 1)
            for i in range(3):
                text_qkv[side, :, i * size : (i + 1) * size] = parts[i]
        if paired:
            send(text_qkv.at[1], text_qkv.at[0], tq_sems, (0,), partner)

    when_active(text_projection)
    if paired:

        @pl.when(jnp.logical_not(active))
        def _():
            arrive(text_qkv.at[0], tq_sems, (0,), partner)

    query[image_rows:, :] = text_qkv[0, :, 0:size]
    key_value[z, image_rows:, :] = text_qkv[0, :, size : 3 * size]
    ring_part(0, 3, 4, kv_part, kv_sems)

    row_max[...] = jnp.full_like(row_max, -1e30)
    row_sum[...] = jnp.zeros_like(row_sum)
    mixed[...] = jnp.zeros_like(mixed)
    factor = float(size) ** (-0.5) * math.log2(math.e)

    def attend(first, last):
        def one(j, carry):
            block = block_at(j)
            scores = lax.dot_general(
                query[...],
                key_value[block, :, 0:size],
                (((1,), (1,)), ((), ())),
                preferred_element_type=F32,
            )
            within = lax.broadcasted_iota(jnp.int32, scores.shape, 1)
            slot = block * text_rows + within - image_rows
            usable = (within < image_rows) | (slot < text_length[0])
            scores = jnp.where(usable, scores, -1e30)
            old = row_max[:, 0:1]
            new = jnp.maximum(old, jnp.max(scores, axis=-1, keepdims=True))
            probs = jnp.exp2((scores - new) * factor)
            fade = jnp.exp2((old - new) * factor)
            row_max[...] = jnp.broadcast_to(new, row_max.shape)
            total = row_sum[:, 0:1] * fade + jnp.sum(probs, axis=-1, keepdims=True)
            row_sum[...] = jnp.broadcast_to(total, row_sum.shape)
            mixed[...] = mixed[...] * fade + jnp.dot(
                probs.astype(BF16),
                key_value[block, :, size : 2 * size],
                preferred_element_type=F32,
            )
            return carry

        lax.fori_loop(first, last, one, 0)

    for d in range(1, half + 1):
        for part in (0, 1):
            ring_part(d, part, 4, kv_part, kv_sems)
        attend(max(2 * d - 3, 0), 2 * d - 2 if d > 1 else 1)
        for part in (2, 3):
            ring_part(d, part, 4, kv_part, kv_sems)
        proj_advance(half + d)
        if d > 1:
            attend(2 * d - 2, 2 * d - 1)
    proj_advance(2 * half + 1)
    attend(nz - 1, nz)

    attended[me] = (mixed[...] / row_sum[:, 0:1]).astype(BF16)

    x_half = nx // 2
    x_right, x_left = {"tensor": wrap(x + 1, nx)}, {"tensor": wrap(x - 1, nx)}

    def x_carried(way, d, part):
        return d < x_half or (part < 2) == (way == RIGHT)

    def x_block(way, d):
        return (wrap(x - d, nx) if way == RIGHT else wrap(x + d, nx)) * nc + c

    def a_part(block, part):
        return attended.at[block, pl.ds(starts[part], starts[part + 1] - starts[part]), :]

    for d in range(0, x_half + 1):
        for part in range(4):
            for way, to in ((RIGHT, x_right), (LEFT, x_left)):
                if not x_carried(way, d, part):
                    continue
                here = a_part(x_block(way, d), part)
                if d > 0:
                    arrive(here, ax_sems, (way, d - 1, part), to)
                if d < x_half and x_carried(way, d + 1, part):
                    send(here, here, ax_sems, (way, d, part), to)
                if d > 0 or way == RIGHT:
                    send(here, here, as_sems, (way, d, part), sibling)

    if paired:
        arrive(other_shares, py_sems, (0,), partner)

    across = 1 - 2 * c
    for d in range(0, x_half + 1):
        for part in range(4):
            for way in (RIGHT, LEFT):
                if x_carried(way, d, part) and (d > 0 or way == RIGHT):
                    arrive(
                        a_part(x_block(way, d) + across, part), as_sems, (way, d, part), sibling
                    )

    out_width = text_out.shape[1]
    image_sum, text_sum = None, None
    for h in range(0, heads, 2):
        rows = jnp.concatenate([attended[h], attended[h + 1]], axis=1)
        image_w = jnp.concatenate([proj_all[h, 0], proj_all[h + 1, 0]], axis=1)
        text_w = jnp.concatenate([proj_all[h, 1], proj_all[h + 1, 1]], axis=1)
        turned = (((1,), (1,)), ((), ()))
        image_term = lax.dot_general(
            rows[:image_rows], image_w, turned, preferred_element_type=F32
        )
        text_term = lax.dot_general(rows[image_rows:], text_w, turned, preferred_element_type=F32)
        image_sum = image_term if image_sum is None else image_sum + image_term
        text_sum = text_term if text_sum is None else text_sum + text_term

    def own_columns(wide):
        return jnp.where(c == 0, wide[:, :out_width], wide[:, out_width:])

    window = pl.ds(pl.multiple_of(x * 2 * out_width, 128), 2 * out_width)
    for tokens, total, out, stream in (
        (image_tokens, image_sum, image_out, 0),
        (text_tokens, text_sum, text_out, 1),
    ):
        gate = own_columns(mod_piece((stream * 3 + 2) * pieces + x))
        base = own_columns(tokens[:, window].astype(F32))
        result = base + gate * total
        out[...] = (jnp.transpose(result) if stream == 0 else result).astype(BF16)

    mod_sent()
    sent(mod_all.at[pl.ds(0, heads - 1)], modx_sems, (0,), sibling)
    blocks = pl.ds(0, nz - 1)
    sent(weights.at[pl.ds(0, (nz - 1) * share), :], w_sems, (0, 0, 0), right)
    sent(proj_z.at[blocks, :, pl.ds(0, share), :], p_sems, (0, 0, 0), right)
    sent(proj_all.at[pl.ds(0, heads - 1), :, pl.ds(0, share), :], px_sems, (0,), sibling)
    sent(key_value.at[blocks], kv_sems, (0, 0, 0), right)
    sent(attended.at[pl.ds(0, nx - 1)], ax_sems, (0, 0, 0), x_right)
    sent(attended.at[pl.ds(0, nx)], as_sems, (0, 0, 0), sibling)
    if paired:
        sent(weights.at[pl.ds(0, (nz - 1) * share), :], wy_sems, (0, 0, 0), partner)
        sent(all_shares, py_sems, (0,), partner)

    def text_sent():
        sent(text_weights.at[pl.ds(0, (nz - 1) * slab), :], t_sems, (0, 0, 0), right)
        if paired:
            sent(text_qkv.at[1], tq_sems, (0,), partner)

    when_active(text_sent)
    if paired:

        @pl.when(jnp.logical_not(active))
        def _():
            sent(both[0], th_sems, (0,), partner)


def hand_out(image, text, image_out, text_out):
    image_out[...] = image[...]
    text_out[...] = text[...]


def solution(mesh):
    nz, nx, nc = mesh.shape["seq"], mesh.shape["tensor"], mesh.shape["sub"]
    paired = mesh.shape["groups"] % 2 == 0
    heads = nx * nc

    def body(
        image_tokens,
        text_tokens,
        timestep,
        text_length,
        time_table,
        mod_weight,
        qkv_image,
        qkv_text,
        norm_gain,
        proj_image,
        proj_text,
    ):
        slab = qkv_image.shape[0]
        gains = norm_gain.reshape(2, 2, 1, norm_gain.shape[-1])
        image_rows, width = image_tokens.shape
        text_rows = text_tokens.shape[0]
        local_rows = image_rows + text_rows
        columns = qkv_image.shape[1]
        size = columns // 3
        out_width = width // heads
        half = nz // 2
        vmem = pl.BlockSpec(memory_space=pltpu.VMEM)
        anywhere = pl.BlockSpec(memory_space=pl.ANY)
        dma = pltpu.SemaphoreType.DMA

        def pair(*shape):
            return dma((1,)), dma(shape)

        results = pl.pallas_call(
            functools.partial(kernel, (nz, nx, nc), paired),
            out_shape=(
                jax.ShapeDtypeStruct((out_width, image_rows), BF16),
                jax.ShapeDtypeStruct((text_rows, out_width), BF16),
            ),
            in_specs=[pl.BlockSpec(memory_space=pltpu.HBM)] * 2 + [anywhere] * 9,
            out_specs=(vmem, vmem),
            scratch_shapes=[
                pltpu.VMEM(image_tokens.shape, BF16),
                pltpu.VMEM(text_tokens.shape, BF16),
                pltpu.VMEM((time_table.shape[0], 2 * slab), BF16),
                pltpu.VMEM(mod_weight.shape, BF16),
                pltpu.VMEM(gains.shape, F32),
                pltpu.VMEM((mod_weight.shape[1] // 128, 1, 128), F32),
                pltpu.VMEM((mod_weight.shape[1] // 128, nz, 1, 128), F32),
                pltpu.VMEM((heads, 1, mod_weight.shape[1]), F32),
                pltpu.VMEM((local_rows, 128), F32),
                pltpu.VMEM((local_rows, 128), F32),
                pltpu.VMEM((image_rows, width), BF16),
                pltpu.VMEM((2 * text_rows, width), BF16),
                pltpu.VMEM((width, columns), BF16),
                pltpu.VMEM((width, columns), BF16),
                pltpu.VMEM((image_rows, columns), F32),
                pltpu.VMEM((2 * text_rows, columns), F32),
                pltpu.VMEM((2, text_rows, columns), BF16),
                pltpu.VMEM((nz, 2, *proj_image.shape[::-1]), BF16),
                pltpu.VMEM((heads, 2, *proj_image.shape[::-1]), BF16),
                pltpu.VMEM((local_rows, size), BF16),
                pltpu.VMEM((nz, local_rows, 2 * size), BF16),
                pltpu.VMEM((local_rows, 128), F32),
                pltpu.VMEM((local_rows, 128), F32),
                pltpu.VMEM((local_rows, size), F32),
                pltpu.VMEM((heads, local_rows, size), BF16),
                pltpu.SMEM((1,), jnp.int32),
                pltpu.SMEM((1,), jnp.int32),
                dma((11,)),
                dma((2, 2, mod_weight.shape[1] // 128)),
                *pair(1),
                *pair(2, half, 2),
                *pair(2, half, 2),
                *pair(2, half, 2),
                *pair(1),
                *pair(1),
                *pair(2, half, 2),
                *pair(1),
                *pair(1),
                *pair(2, half, 4),
                *pair(2, nx // 2, 4),
                *pair(2, nx // 2 + 1, 4),
            ],
            compiler_params=pltpu.CompilerParams(
                collective_id=0, has_side_effects=True, vmem_limit_bytes=56 * 1024 * 1024
            ),
        )(
            text_length,
            timestep,
            image_tokens,
            text_tokens,
            time_table,
            mod_weight,
            gains,
            qkv_image,
            qkv_text,
            proj_image.T,
            proj_text.T,
        )
        image_turned, text_out = pl.pallas_call(
            hand_out,
            out_shape=tuple(jax.ShapeDtypeStruct(r.shape, r.dtype) for r in results),
            in_specs=[vmem] * 2,
            out_specs=(vmem, vmem),
        )(*results)
        return image_turned.T, text_out

    return jax.shard_map(
        body,
        mesh=mesh,
        in_specs=(
            P(("groups", "seq"), None),
            P(("groups", "seq"), None),
            P("groups"),
            P("groups"),
            P(),
            P("seq", ("tensor", "sub")),
            P("seq", ("tensor", "sub")),
            P("seq", ("tensor", "sub")),
            P(None, None, ("tensor", "sub"), None),
            P(("tensor", "sub"), "seq"),
            P(("tensor", "sub"), "seq"),
        ),
        out_specs=(
            P(("groups", "seq"), ("tensor", "sub")),
            P(("groups", "seq"), ("tensor", "sub")),
        ),
        check_vma=False,
    )
```
